256 devices in a mesh: gx: 16 (over y_hi, z), gy: 4 (over y_lo, core), gz: 4 (over x).
Axes of the slice: x: 4, y: 4 (y_hi: 2, y_lo: 2; y = y_hi * 2 + y_lo), z: 8, core: 2. Of those that a mesh axis runs over, the one named last changes fastest.
Arguments:
- flow_pops: float32 [19, 128, 32, 512], P(None, 'gx', 'gy', 'gz'), may hold values from 0 to 0.6, as said below
- heat_pops: float32 [7, 128, 32, 512], P(None, 'gx', 'gy', 'gz'), may hold values from -0.2 to 0.2
Outputs:
- flow_out: float32 [19, 128, 32, 512], P(None, 'gx', 'gy', 'gz')
- heat_out: float32 [7, 128, 32, 512], P(None, 'gx', 'gy', 'gz')
- nusselt: float32 [], replicated
The draws below stay inside these ranges and needn't reach their ends.
Inputs may be any that keep to these rules, and one draw needn't show every extreme that they name: `flow_pops`: positive flow populations.
All inputs are finite; a program needn't handle non-finite values.
Results may differ from the reference program's by a relative error of at most 0.0001.
Values sent between devices are 32-bit elements; how exact they have to be, the bound alone decides.
A program may use at most 64 MiB of HBM per device.

```python
import jax
import jax.numpy as jnp
import numpy as np

STEPS = 3
NX = 128
NY = 32
NZ = 512


FLOW_WEIGHT = np.array([1.0 / 3.0] + [1.0 / 18.0] * 6 + [1.0 / 36.0] * 12)


D3Q7_QUADRATURE = np.array([0.25] + [0.125] * 6)


def draw_flow_pops(key, part):
    weight = jnp.asarray(FLOW_WEIGHT, jnp.float32).reshape(19, 1, 1, 1)
    factor = jax.random.uniform(key, (19, NX, NY, NZ), jnp.float32, 0.8, 1.2)
    return (weight * factor).astype(jnp.float32)


def draw_heat_pops(key, part):
    weight = jnp.asarray(D3Q7_QUADRATURE, jnp.float32).reshape(7, 1, 1, 1)
    noise = jax.random.uniform(jax.random.fold_in(key, 21), (7, NX, NY, NZ), jnp.float32, -0.1, 0.1)
    cell_temp = jax.random.uniform(jax.random.fold_in(key, 23), (1, NX, NY, NZ), jnp.float32, -0.4, 0.4)
    return (weight * (cell_temp + noise)).astype(jnp.float32)


def setup_inputs(seed: int = 0) -> dict:
    splits = jax.random.split(jax.random.key(seed), 3)
    flow_pops = draw_flow_pops(jax.random.fold_in(splits[2], 71), 0)
    heat_pops = draw_heat_pops(jax.random.fold_in(splits[2], 71), 0)
    return dict(flow_pops=flow_pops, heat_pops=heat_pops)


FLOW_SET = np.array([[0, 0, 0], [1, 0, 0], [-1, 0, 0], [0, 1, 0], [0, -1, 0], [0, 0, 1], [0, 0, -1], [1, 1, 0], [-1, -1, 0], [1, -1, 0], [-1, 1, 0], [1, 0, 1], [-1, 0, -1], [1, 0, -1], [-1, 0, 1], [0, 1, 1], [0, -1, -1], [0, 1, -1], [0, -1, 1]])
FLOW_WEIGHT = np.array([1.0 / 3.0] + [1.0 / 18.0] * 6 + [1.0 / 36.0] * 12)
D3Q7_QUADRATURE = np.array([0.25] + [0.125] * 6)
LATTICE = np.concatenate([FLOW_SET, FLOW_SET[:7]], axis=0)
WEIGHTS = np.concatenate([FLOW_WEIGHT, D3Q7_QUADRATURE])
OPPOSITE = np.array([[r for r in range(19) if (FLOW_SET[r] == -FLOW_SET[q]).all()][0] for q in range(19)] + [19 + [r for r in range(7) if (FLOW_SET[r] == -FLOW_SET[q]).all()][0] for q in range(7)])
TAU_FLOW = 0.6
TAU_HEAT = 0.7
GRAVITY_LIFT = 0.01
HOT_WALL = 0.5
COLD_WALL = -0.5
DIFFUSIVITY = (TAU_HEAT - 0.5) / 4.0


def stacked_subarray(values, count):
    return jnp.asarray(values[:count], jnp.float32).reshape(count, 1, 1, 1)


def hydrodynamic_observables(momentum_populations, energy_populations):
    mass_per_site = jnp.sum(momentum_populations, axis=0)
    site_warmth = jnp.sum(energy_populations, axis=0)
    gravity_direction_push = GRAVITY_LIFT * mass_per_site * site_warmth
    speed_xaxis_component = jnp.sum(stacked_subarray(FLOW_SET[:, 0], 19) * momentum_populations, axis=0) / mass_per_site
    speed_yaxis_component = jnp.sum(stacked_subarray(FLOW_SET[:, 1], 19) * momentum_populations, axis=0) / mass_per_site
    speed_zaxis_component = (jnp.sum(stacked_subarray(FLOW_SET[:, 2], 19) * momentum_populations, axis=0) + 0.5 * gravity_direction_push) / mass_per_site
    return mass_per_site, site_warmth, gravity_direction_push, speed_xaxis_component, speed_yaxis_component, speed_zaxis_component


def collide(momentum_populations, energy_populations):
    mass_per_site, site_warmth, gravity_direction_push, speed_xaxis_component, speed_yaxis_component, speed_zaxis_component = hydrodynamic_observables(momentum_populations, energy_populations)
    dir_z = stacked_subarray(FLOW_SET[:, 2], 19)
    projected_onto_link = stacked_subarray(FLOW_SET[:, 0], 19) * speed_xaxis_component + stacked_subarray(FLOW_SET[:, 1], 19) * speed_yaxis_component + dir_z * speed_zaxis_component
    speed_sq = speed_xaxis_component * speed_xaxis_component + speed_yaxis_component * speed_yaxis_component + speed_zaxis_component * speed_zaxis_component
    weight = stacked_subarray(FLOW_WEIGHT, 19)
    equil = weight * mass_per_site * (1.0 + 3.0 * projected_onto_link + 4.5 * projected_onto_link * projected_onto_link - 1.5 * speed_sq)
    source = (1.0 - 0.5 / TAU_FLOW) * weight * (3.0 * (dir_z - speed_zaxis_component) + 9.0 * projected_onto_link * dir_z) * gravity_direction_push
    flow_post = momentum_populations - (momentum_populations - equil) / TAU_FLOW + source
    warmth_rest_distribution = stacked_subarray(D3Q7_QUADRATURE, 7) * site_warmth * (1.0 + 4.0 * projected_onto_link[:7])
    heat_post = energy_populations - (energy_populations - warmth_rest_distribution) / TAU_HEAT
    return jnp.concatenate([flow_post, heat_post], axis=0)


def apply_walls(read, post, is_bottom, is_top):
    result = []
    for member in range(26):
        single = read[member]
        dir_z = int(LATTICE[member, 2])
        if dir_z != 0:
            plane = 0 if dir_z == 1 else single.shape[2] - 1
            flag = is_bottom if dir_z == 1 else is_top
            wall_temp = HOT_WALL if dir_z == 1 else COLD_WALL
            back = post[int(OPPOSITE[member])][:, :, plane]
            if member >= 19:
                back = -back + 2.0 * float(WEIGHTS[member]) * wall_temp
            single = single.at[:, :, plane].set(jnp.where(flag, back, single[:, :, plane]))
        result.append(single)
    return jnp.stack(result)


def local_flux(momentum_populations, energy_populations):
    mass_per_site, site_warmth, gravity_direction_push, speed_xaxis_component, speed_yaxis_component, speed_zaxis_component = hydrodynamic_observables(momentum_populations, energy_populations)
    return jnp.sum(speed_zaxis_component * site_warmth)


def reference(flow_pops, heat_pops):
    momentum_populations, energy_populations = flow_pops, heat_pops
    for period in range(STEPS):
        post = collide(momentum_populations, energy_populations)
        result = []
        for member in range(26):
            single = jnp.roll(post[member], int(LATTICE[member, 0]), 0)
            single = jnp.roll(single, int(LATTICE[member, 1]), 1)
            dir_z = int(LATTICE[member, 2])
            zeros = jnp.zeros(single.shape[:2] + (1,), jnp.float32)
            if dir_z == 1:
                single = jnp.concatenate([zeros, single[:, :, :-1]], axis=2)
            elif dir_z == -1:
                single = jnp.concatenate([single[:, :, 1:], zeros], axis=2)
            result.append(single)
        read = apply_walls(jnp.stack(result), post, True, True)
        momentum_populations, energy_populations = read[:19], read[19:]
    total = local_flux(momentum_populations, energy_populations)
    nusselt = 1.0 + NZ / (DIFFUSIVITY * (HOT_WALL - COLD_WALL)) * total / (NX * NY * NZ)
    return momentum_populations, energy_populations, nusselt.astype(jnp.float32)
```

```python
import functools

import jax
import jax.numpy as jnp
import numpy as np
from jax import lax
from jax.experimental import pallas as pl
from jax.experimental.pallas import tpu as pltpu
from jax.sharding import PartitionSpec as P

MESH = pl.DeviceIdType.MESH
STEPS = 3
AXES = ("gx", "gy", "gz")

FLOW_SET = [
    (0, 0, 0),
    (1, 0, 0),
    (-1, 0, 0),
    (0, 1, 0),
    (0, -1, 0),
    (0, 0, 1),
    (0, 0, -1),
    (1, 1, 0),
    (-1, -1, 0),
    (1, -1, 0),
    (-1, 1, 0),
    (1, 0, 1),
    (-1, 0, -1),
    (1, 0, -1),
    (-1, 0, 1),
    (0, 1, 1),
    (0, -1, -1),
    (0, 1, -1),
    (0, -1, 1),
]
LATTICE = FLOW_SET + FLOW_SET[:7]
FLOWS = len(FLOW_SET)
POPS = len(LATTICE)
TAU_FLOW = 0.6
TAU_HEAT = 0.7
GRAVITY_LIFT = 0.01
HOT_WALL = 0.5
COLD_WALL = -0.5
DIFFUSIVITY = (TAU_HEAT - 0.5) / 4.0


def opposite(q):
    c = tuple(-v for v in LATTICE[q])
    return FLOW_SET.index(c) + (FLOWS if q >= FLOWS else 0)


def movers(axis, sign):
    return [q for q in range(POPS) if LATTICE[q][axis] == sign]


XP, XM = movers(0, 1), movers(0, -1)
YM = {1: movers(1, 1), -1: movers(1, -1)}
ZM = {1: movers(2, 1), -1: movers(2, -1)}
FACE = len(XP)
ORDER = XP + XM + [q for q in range(POPS) if LATTICE[q][0] == 0]
POS = {q: i for i, q in enumerate(ORDER)}
XY = [(q, LATTICE[q]) for q in range(FLOWS) if LATTICE[q][0] != 0 and LATTICE[q][1] != 0]
XY_SLOT = {q: i for i, (q, _) in enumerate(XY)}
ZOFF = [(0, 0), (1, 0), (-1, 0), (0, 1), (0, -1)]
LANE0 = 8


def messages():
    out = [("x", 1, (1, 0, 0)), ("x", -1, (-1, 0, 0)), ("y", 1, (0, 1, 0)), ("y", -1, (0, -1, 0))]
    out += [("xy", q, c) for q, c in XY]
    out += [("z", (cz, i), (dx, dy, cz)) for cz in (1, -1) for i, (dx, dy) in enumerate(ZOFF)]
    return out


MESSAGES = messages()


def collide(f):
    s, d = {}, {}
    for q in range(1, FLOWS, 2):
        s[q] = f[q] + f[q + 1]
        d[q] = f[q] - f[q + 1]
    rho = (((s[1] + s[3]) + (s[5] + s[7])) + ((s[9] + s[11]) + (s[13] + s[15]))) + (s[17] + f[0])
    jx = (d[1] + d[7]) + (d[9] + d[11]) + d[13]
    jy = (d[3] + d[7]) + (d[15] + d[17]) - d[9]
    jz = (d[5] + d[11]) + (d[15] - d[13]) - d[17]
    g = [f[FLOWS + i] for i in range(7)]
    warmth = ((g[0] + g[1]) + (g[2] + g[3])) + ((g[4] + g[5]) + g[6])
    force = GRAVITY_LIFT * rho * warmth
    inv = 1.0 / rho
    ux = jx * inv
    uy = jy * inv
    uz = (jz + 0.5 * force) * inv

    w2 = 1.0 / 36.0
    keep = 1.0 - 1.0 / TAU_FLOW
    r = (w2 / TAU_FLOW) * rho
    sf = (w2 * (1.0 - 0.5 / TAU_FLOW)) * force
    r3 = 3.0 * r
    rx, ry, rz = r3 * ux, r3 * uy, r3 * uz
    sf3 = 3.0 * sf
    ax, ay, az = rx, ry, rz + sf3
    bx, by, bz = 1.5 * rx, 1.5 * ry, 1.5 * rz + 3.0 * sf3
    qx, qy, qz = ux * bx, uy * by, uz * bz
    usq = rx * ux + ry * uy + rz * uz
    base = r - 0.5 * usq - sf3 * uz
    cxy = ux * by + uy * bx
    cxz = ux * bz + uz * bx
    cyz = uy * bz + uz * by

    out = {0: keep * f[0] + 12.0 * base}

    def pair(q, even, odd):
        out[q] = keep * f[q] + (even + odd)
        out[q + 1] = keep * f[q + 1] + (even - odd)

    pair(1, 2.0 * (base + qx), 2.0 * ax)
    pair(3, 2.0 * (base + qy), 2.0 * ay)
    pair(5, 2.0 * (base + qz), 2.0 * az)
    exy = base + (qx + qy)
    exz = base + (qx + qz)
    eyz = base + (qy + qz)
    pair(7, exy + cxy, ax + ay)
    pair(9, exy - cxy, ax - ay)
    pair(11, exz + cxz, ax + az)
    pair(13, exz - cxz, ax - az)
    pair(15, eyz + cyz, ay + az)
    pair(17, eyz - cyz, ay - az)

    keep_heat = 1.0 - 1.0 / TAU_HEAT
    t8 = (0.125 / TAU_HEAT) * warmth
    t2 = 4.0 * t8
    out[FLOWS] = keep_heat * g[0] + 2.0 * t8
    for i, u in ((1, ux), (3, uy), (5, uz)):
        odd = t2 * u
        out[FLOWS + i] = keep_heat * g[i] + (t8 + odd)
        out[FLOWS + i + 1] = keep_heat * g[i + 1] + (t8 - odd)
    return out


def flux(f):
    total = lambda values: functools.reduce(lambda a, b: a + b, values)
    rho = total([f[q] for q in range(FLOWS)])
    jz = total([f[q] for q in range(FLOWS) if LATTICE[q][2] == 1]) - total(
        [f[q] for q in range(FLOWS) if LATTICE[q][2] == -1]
    )
    warmth = total([f[q] for q in range(FLOWS, POPS)])
    force = GRAVITY_LIFT * rho * warmth
    return (jz + 0.5 * force) / rho * warmth


def kernel(
    shape,
    sizes,
    flow_in,
    heat_in,
    flow_out,
    heat_out,
    nusselt,
    held,
    post,
    ysend,
    yrecv,
    ydiag,
    zsend,
    zrecv,
    yedge,
    red_a,
    red_b,
    in_sem,
    out_sem,
    send_sem,
    recv_sem,
    send_a,
    recv_a,
    send_b,
    recv_b,
):
    nx, ny, nz = shape
    planes, rows, lanes = sizes
    me = tuple(lax.axis_index(a) for a in AXES)

    def at(off):
        return tuple(
            m if d == 0 else lax.rem(m + (d % n), n) for m, d, n in zip(me, off, shape)
        )

    loads = [
        pltpu.make_async_copy(flow_in, held.at[pl.ds(0, FLOWS)], in_sem.at[0]),
        pltpu.make_async_copy(heat_in, held.at[pl.ds(FLOWS, 7)], in_sem.at[1]),
    ]
    for c in loads:
        c.start()

    offsets = {tuple(d % n for d, n in zip(off, shape)) for _, _, off in MESSAGES}
    offsets |= {(0, dy, dz) for dy in range(ny) for dz in range(nz)}
    offsets |= {(dx, 0, 0) for dx in range(nx)}
    offsets -= {(0, 0, 0)}
    barrier = pltpu.get_barrier_semaphore()
    for off in sorted(offsets):
        pl.semaphore_signal(barrier, inc=1, device_id=at(off), device_id_type=MESH)

    lane = lax.broadcasted_iota(jnp.int32, (rows, lanes), 1)
    row = lax.broadcasted_iota(jnp.int32, (rows, lanes), 0)
    is_bottom = me[2] == 0
    is_top = me[2] == nz - 1
    end_lane = {1: lane == 0, -1: lane == lanes - 1}
    wall = {1: jnp.logical_and(end_lane[1], is_bottom), -1: jnp.logical_and(end_lane[-1], is_top)}
    end_row = {1: row == 0, -1: row == rows - 1}
    far_row = {1: row == rows - 1, -1: row == 0}

    def turn(v, c, axis):
        n = rows if axis == 0 else lanes
        return pltpu.roll(v, 1 if c == 1 else n - 1, axis)

    def plane(x):
        return pl.ds(pl.multiple_of((x + 1) * rows, rows), rows)

    def keep(s, x, out, packed):
        for q in range(POPS):
            post[s, POS[q], plane(x), :] = out[q]
        result = []
        for cz, tile in zip((1, -1), packed):
            for j, q in enumerate(ZM[cz]):
                k = LANE0 + j * planes + x
                tile = jnp.where(lane == k, pltpu.roll(out[q], k + (1 if cz == 1 else 0), 1), tile)
            result.append(tile)
        return tuple(result)

    def copy(s, m):
        kind, slot, off = MESSAGES[m]
        if kind == "x":
            group = pl.ds(0 if slot == 1 else FACE, FACE)
            src, dst = (planes, 0) if slot == 1 else (1, planes + 1)
            src = post.at[s, group, pl.ds(src * rows, rows)]
            dst = post.at[s, group, pl.ds(dst * rows, rows)]
        elif kind == "y":
            src, dst = (b.at[s, 0 if slot == 1 else 1] for b in (ysend, yrecv))
        elif kind == "xy":
            cy = off[1]
            src = ysend.at[s, 0 if cy == 1 else 1, YM[cy].index(slot)]
            dst = ydiag.at[s, XY_SLOT[slot]]
        else:
            cz, i = slot
            src = zsend.at[s, 0 if cz == 1 else 1]
            dst = zrecv.at[s, 0 if cz == 1 else 1, i]
        return pltpu.make_async_remote_copy(
            src_ref=src,
            dst_ref=dst,
            send_sem=send_sem.at[s, m],
            recv_sem=recv_sem.at[s, m],
            device_id=at(off),
            device_id_type=MESH,
        )

    def of_kind(dz):
        return [m for m, (_, _, off) in enumerate(MESSAGES) if off[2] == dz]

    def send(s, packed):
        for i, cy in enumerate((1, -1)):
            first = rows + (rows - 1 if cy == 1 else 0)
            for j, q in enumerate(YM[cy]):
                ysend[s, i, j] = post[s, POS[q], pl.ds(first, planes, stride=rows), :]
        zsend[s, 0] = packed[0]
        zsend[s, 1] = packed[1]

    def start(s):
        for m in of_kind(0):
            copy(s, m).start()

        @pl.when(jnp.logical_not(is_top))
        def _():
            for m in of_kind(1):
                copy(s, m).start()

        @pl.when(jnp.logical_not(is_bottom))
        def _():
            for m in of_kind(-1):
                copy(s, m).start()

    def receive(s):
        for m in of_kind(0):
            copy(s, m).wait_recv()

        @pl.when(jnp.logical_not(is_bottom))
        def _():
            for m in of_kind(1):
                copy(s, m).wait_recv()

        @pl.when(jnp.logical_not(is_top))
        def _():
            for m in of_kind(-1):
                copy(s, m).wait_recv()

    def drain(s):
        for m in of_kind(0):
            copy(s, m).wait_send()

        @pl.when(jnp.logical_not(is_top))
        def _():
            for m in of_kind(1):
                copy(s, m).wait_send()

        @pl.when(jnp.logical_not(is_bottom))
        def _():
            for m in of_kind(-1):
                copy(s, m).wait_send()

    def edges(s):
        for i, cy in enumerate((1, -1)):
            for j, q in enumerate(YM[cy]):
                cx = LATTICE[q][0]
                tile = yrecv[s, i, j]
                if cx:
                    tile = turn(jnp.where(far_row[cx], ydiag[s, XY_SLOT[q]], tile), cx, 0)
                yedge[s, i, j] = tile
        tiles = {}
        for i, cz in enumerate((1, -1)):
            own = zrecv[s, i, 0]
            tile = own
            for j, q in enumerate(ZM[cz]):
                cx, cy, _ = LATTICE[q]
                if cx == 0 and cy == 0:
                    continue
                low = LANE0 + j * planes
                other = zrecv[s, i, ZOFF.index((cx, cy))]
                if cx:
                    near = low + (0 if cx == 1 else planes - 1)
                    back = (lanes - planes + 1) if cx == 1 else planes - 1
                    moved = jnp.where(lane == near, pltpu.roll(other, back, 1), turn(own, cx, 1))
                else:
                    moved = turn(jnp.where(far_row[cy], other, own), cy, 0)
                tile = jnp.where(jnp.logical_and(lane >= low, lane < low + planes), moved, tile)
            tiles[cz] = tile
        return tiles

    def stream(s, x, tiles):
        f = {}
        for q in range(POPS):
            cx, cy, cz = LATTICE[q]
            v = post[s, POS[q], plane(x - cx), :]
            if cy:
                i, j = (0 if cy == 1 else 1), YM[cy].index(q)
                edge = jnp.broadcast_to(yedge[s, i, j, pl.ds(x, 1), :], (rows, lanes))
                v = jnp.where(end_row[cy], edge, turn(v, cy, 0))
            if cz:
                k = LANE0 + ZM[cz].index(q) * planes + x
                edge = pltpu.roll(tiles[cz], (lanes if cz == 1 else lanes - 1) - k, 1)
                back = post[s, POS[opposite(q)], plane(x), :]
                if q >= FLOWS:
                    back = 0.25 * (HOT_WALL if cz == 1 else COLD_WALL) - back
                v = jnp.where(wall[cz], back, jnp.where(end_lane[cz], edge, turn(v, cz, 1)))
            f[q] = v
        return f

    blank = jnp.zeros((rows, lanes), jnp.float32)

    for c in loads:
        c.wait()

    def first(x, packed):
        at_x = pl.ds(pl.multiple_of(x * rows, rows), rows)
        return keep(0, x, collide({q: held[q, at_x, :] for q in range(POPS)}), packed)

    send(0, lax.fori_loop(0, planes, first, (blank, blank)))
    pl.semaphore_wait(barrier, len(offsets))
    start(0)

    for s in range(1, STEPS):
        receive(s - 1)
        tiles = edges(s - 1)

        def middle(x, packed, s=s, tiles=tiles):
            return keep(s, x, collide(stream(s - 1, x, tiles)), packed)

        send(s, lax.fori_loop(0, planes, middle, (blank, blank)))
        start(s)

    receive(STEPS - 1)
    tiles = edges(STEPS - 1)

    def last(x, acc):
        f = stream(STEPS - 1, x, tiles)
        at_x = pl.ds(pl.multiple_of(x * rows, rows), rows)
        for q in range(POPS):
            held[q, at_x, :] = f[q]
        return acc + flux(f)

    acc = lax.fori_loop(0, planes, last, blank)
    stores = [
        pltpu.make_async_copy(held.at[pl.ds(0, FLOWS)], flow_out, out_sem.at[0]),
        pltpu.make_async_copy(held.at[pl.ds(FLOWS, 7)], heat_out, out_sem.at[1]),
    ]
    for c in stores:
        c.start()

    def exchange(value, buf, index, peers, sends, recvs):
        buf[index] = value
        count = buf.shape[0]

        def to(d):
            return pltpu.make_async_remote_copy(
                src_ref=buf.at[index],
                dst_ref=buf.at[index],
                send_sem=sends.at[d],
                recv_sem=recvs.at[d],
                device_id=peers[d],
                device_id_type=MESH,
            )

        for d in range(1, count):
            to(d).start()
        for d in range(1, count):
            to(d).wait_recv()
        total = buf[0]
        for d in range(1, count):
            total = total + buf[d]
        for d in range(1, count):
            to(d).wait_send()
        return total

    part = jnp.sum(acc, axis=0, keepdims=True)
    peers = [at((0, d // nz, d % nz)) for d in range(ny * nz)]
    part = exchange(part, red_a, me[1] * nz + me[2], peers, send_a, recv_a)
    peers = [at((d, 0, 0)) for d in range(nx)]
    part = exchange(part, red_b, me[0], peers, send_b, recv_b)
    total = jnp.sum(part)
    cells = nx * planes * ny * rows * nz * lanes
    height = nz * lanes
    nusselt[0, 0] = 1.0 + (height / (DIFFUSIVITY * (HOT_WALL - COLD_WALL)) / cells) * total

    for s in range(STEPS):
        drain(s)
    for c in stores:
        c.wait()


def per_device(shape, flow_pops, heat_pops):
    nx, ny, nz = shape
    _, planes, rows, lanes = flow_pops.shape
    flat = (planes * rows, lanes)
    dma = pltpu.SemaphoreType.DMA
    tile = (rows, lanes)
    vmem = lambda *dims: pltpu.VMEM(dims, jnp.float32)
    flow, heat, nusselt = pl.pallas_call(
        functools.partial(kernel, shape, (planes, rows, lanes)),
        out_shape=(
            jax.ShapeDtypeStruct((FLOWS,) + flat, jnp.float32),
            jax.ShapeDtypeStruct((7,) + flat, jnp.float32),
            jax.ShapeDtypeStruct((1, 1), jnp.float32),
        ),
        in_specs=[pl.BlockSpec(memory_space=pl.ANY)] * 2,
        out_specs=(
            pl.BlockSpec(memory_space=pl.ANY),
            pl.BlockSpec(memory_space=pl.ANY),
            pl.BlockSpec(memory_space=pltpu.SMEM),
        ),
        scratch_shapes=[
            vmem(POPS, *flat),
            vmem(STEPS, POPS, (planes + 2) * rows, lanes),
            vmem(STEPS, 2, FACE, *tile),
            vmem(STEPS, 2, FACE, *tile),
            vmem(STEPS, len(XY), *tile),
            vmem(STEPS, 2, *tile),
            vmem(STEPS, 2, len(ZOFF), *tile),
            vmem(STEPS, 2, FACE, *tile),
            vmem(ny * nz, 1, lanes),
            vmem(nx, 1, lanes),
            dma((2,)),
            dma((2,)),
            dma((STEPS, len(MESSAGES))),
            dma((STEPS, len(MESSAGES))),
            dma((ny * nz,)),
            dma((ny * nz,)),
            dma((nx,)),
            dma((nx,)),
        ],
        compiler_params=pltpu.CompilerParams(collective_id=0, has_side_effects=True),
        name="lattice_steps",
    )(flow_pops.reshape((FLOWS,) + flat), heat_pops.reshape((7,) + flat))
    return flow.reshape(flow_pops.shape), heat.reshape(heat_pops.shape), nusselt.reshape(())


def solution(mesh):
    shape = tuple(mesh.shape[a] for a in AXES)
    spec = P(None, *AXES)
    return jax.shard_map(
        functools.partial(per_device, shape),
        mesh=mesh,
        in_specs=(spec, spec),
        out_specs=(spec, spec, P()),
        check_vma=False,
    )
```

```python
import functools

import jax
import jax.numpy as jnp
import numpy as np
from jax import lax
from jax.experimental import pallas as pl
from jax.experimental.pallas import tpu as pltpu
from jax.sharding import PartitionSpec as P

MESH = pl.DeviceIdType.MESH
STEPS = 3
AXES = ("gx", "gy", "gz")

FLOW_SET = [
    (0, 0, 0),
    (1, 0, 0),
    (-1, 0, 0),
    (0, 1, 0),
    (0, -1, 0),
    (0, 0, 1),
    (0, 0, -1),
    (1, 1, 0),
    (-1, -1, 0),
    (1, -1, 0),
    (-1, 1, 0),
    (1, 0, 1),
    (-1, 0, -1),
    (1, 0, -1),
    (-1, 0, 1),
    (0, 1, 1),
    (0, -1, -1),
    (0, 1, -1),
    (0, -1, 1),
]
LATTICE = FLOW_SET + FLOW_SET[:7]
FLOWS = len(FLOW_SET)
POPS = len(LATTICE)
TAU_FLOW = 0.6
TAU_HEAT = 0.7
GRAVITY_LIFT = 0.01
HOT_WALL = 0.5
COLD_WALL = -0.5
DIFFUSIVITY = (TAU_HEAT - 0.5) / 4.0


def opposite(q):
    c = tuple(-v for v in LATTICE[q])
    return FLOW_SET.index(c) + (FLOWS if q >= FLOWS else 0)


def movers(axis, sign):
    return [q for q in range(POPS) if LATTICE[q][axis] == sign]


XP, XM = movers(0, 1), movers(0, -1)
YM = {1: movers(1, 1), -1: movers(1, -1)}
ZM = {1: movers(2, 1), -1: movers(2, -1)}
FACE = len(XP)
ORDER = XP + XM + [q for q in range(POPS) if LATTICE[q][0] == 0]
POS = {q: i for i, q in enumerate(ORDER)}
XY = [q for q in range(FLOWS) if LATTICE[q][0] != 0 and LATTICE[q][1] != 0]
XZ = [q for q in range(FLOWS) if LATTICE[q][0] != 0 and LATTICE[q][2] != 0]
LANE0 = 8


def messages():
    out = [("x", 1, (1, 0, 0)), ("x", -1, (-1, 0, 0))]
    out += [("xz", q, LATTICE[q]) for q in XZ]
    out += [("xy", q, LATTICE[q]) for q in XY]
    out += [("z", (cz, cy), (0, cy, cz)) for cz in (1, -1) for cy in (1, -1, 0)]
    out += [("y", 1, (0, 1, 0)), ("y", -1, (0, -1, 0))]
    return out


MESSAGES = messages()
END_PLANES = ("x", "xy", "xz")
ALL_PLANES = ("y", "z")


def collide(f):
    s, d = {}, {}
    for q in range(1, FLOWS, 2):
        s[q] = f[q] + f[q + 1]
        d[q] = f[q] - f[q + 1]
    rho = (((s[1] + s[3]) + (s[5] + s[7])) + ((s[9] + s[11]) + (s[13] + s[15]))) + (s[17] + f[0])
    jx = (d[1] + d[7]) + (d[9] + d[11]) + d[13]
    jy = (d[3] + d[7]) + (d[15] + d[17]) - d[9]
    jz = (d[5] + d[11]) + (d[15] - d[13]) - d[17]
    g = [f[FLOWS + i] for i in range(7)]
    warmth = ((g[0] + g[1]) + (g[2] + g[3])) + ((g[4] + g[5]) + g[6])
    force = GRAVITY_LIFT * rho * warmth
    inv = 1.0 / rho
    ux = jx * inv
    uy = jy * inv
    uz = (jz + 0.5 * force) * inv

    w2 = 1.0 / 36.0
    keep = 1.0 - 1.0 / TAU_FLOW
    r = (w2 / TAU_FLOW) * rho
    sf = (w2 * (1.0 - 0.5 / TAU_FLOW)) * force
    r3 = 3.0 * r
    rx, ry, rz = r3 * ux, r3 * uy, r3 * uz
    sf3 = 3.0 * sf
    ax, ay, az = rx, ry, rz + sf3
    bx, by, bz = 1.5 * rx, 1.5 * ry, 1.5 * rz + 3.0 * sf3
    qx, qy, qz = ux * bx, uy * by, uz * bz
    usq = rx * ux + ry * uy + rz * uz
    base = r - 0.5 * usq - sf3 * uz
    cxy = ux * by + uy * bx
    cxz = ux * bz + uz * bx
    cyz = uy * bz + uz * by

    out = {0: keep * f[0] + 12.0 * base}

    def pair(q, even, odd):
        out[q] = keep * f[q] + (even + odd)
        out[q + 1] = keep * f[q + 1] + (even - odd)

    pair(1, 2.0 * (base + qx), 2.0 * ax)
    pair(3, 2.0 * (base + qy), 2.0 * ay)
    pair(5, 2.0 * (base + qz), 2.0 * az)
    exy = base + (qx + qy)
    exz = base + (qx + qz)
    eyz = base + (qy + qz)
    pair(7, exy + cxy, ax + ay)
    pair(9, exy - cxy, ax - ay)
    pair(11, exz + cxz, ax + az)
    pair(13, exz - cxz, ax - az)
    pair(15, eyz + cyz, ay + az)
    pair(17, eyz - cyz, ay - az)

    keep_heat = 1.0 - 1.0 / TAU_HEAT
    t8 = (0.125 / TAU_HEAT) * warmth
    t2 = 4.0 * t8
    out[FLOWS] = keep_heat * g[0] + 2.0 * t8
    for i, u in ((1, ux), (3, uy), (5, uz)):
        odd = t2 * u
        out[FLOWS + i] = keep_heat * g[i] + (t8 + odd)
        out[FLOWS + i + 1] = keep_heat * g[i + 1] + (t8 - odd)
    return out


def flux(f):
    total = lambda values: functools.reduce(lambda a, b: a + b, values)
    rho = total([f[q] for q in range(FLOWS)])
    jz = total([f[q] for q in range(FLOWS) if LATTICE[q][2] == 1]) - total(
        [f[q] for q in range(FLOWS) if LATTICE[q][2] == -1]
    )
    warmth = total([f[q] for q in range(FLOWS, POPS)])
    force = GRAVITY_LIFT * rho * warmth
    return (jz + 0.5 * force) / rho * warmth


def kernel(
    shape,
    sizes,
    flow_in,
    heat_in,
    flow_out,
    heat_out,
    nusselt,
    held,
    post,
    ysend,
    yrecv,
    ydiag,
    zsend,
    zrecv,
    zdiag,
    part,
    parts,
    total,
    in_sem,
    send_sem,
    recv_sem,
    part_send,
    part_recv,
    total_send,
    total_recv,
):
    nx, ny, nz = shape
    planes, rows, lanes = sizes
    me = tuple(lax.axis_index(a) for a in AXES)
    count = nx * ny * nz
    group = ny * nz
    roots = (nx // 4) * group
    my_index = me[0] * group + me[1] * nz + me[2]
    is_root = me[0] < nx // 4

    def at(off):
        return tuple(m if d == 0 else lax.rem(m + (d % n), n) for m, d, n in zip(me, off, shape))

    offsets = [off for off in np.ndindex(3, 3, 3) if off != (1, 1, 1)]
    offsets = [tuple(d - 1 for d in off) for off in offsets if 1 in off]
    barrier = pltpu.get_barrier_semaphore()
    for off in offsets:
        pl.semaphore_signal(barrier, inc=1, device_id=at(off), device_id_type=MESH)

    inner, ends = range(1, planes - 1), (0, planes - 1)
    blocks = [(0, 1), (planes - 1, 1), (1, planes - 2)]
    loads = []
    for i, (x, n) in enumerate(blocks):
        some = pl.ds(x * rows, n * rows)
        for j, (ref, low, n) in enumerate(((flow_in, 0, FLOWS), (heat_in, FLOWS, 7))):
            loads.append(
                pltpu.make_async_copy(ref.at[:, some], held.at[pl.ds(low, n), some], in_sem.at[2 * i + j])
            )
    for c in loads:
        c.start()

    @pl.when(is_root)
    def _():
        def tell(d, carry):
            pl.semaphore_signal(
                barrier,
                inc=1,
                device_id=lax.rem(my_index + d, count),
                device_id_type=pl.DeviceIdType.LOGICAL,
            )
            return carry

        lax.fori_loop(1, count, tell, 0)

    lane = lax.broadcasted_iota(jnp.int32, (rows, lanes), 1)
    row = lax.broadcasted_iota(jnp.int32, (rows, lanes), 0)
    is_bottom = me[2] == 0
    is_top = me[2] == nz - 1
    end_lane = {1: lane == 0, -1: lane == lanes - 1}
    wall = {1: jnp.logical_and(end_lane[1], is_bottom), -1: jnp.logical_and(end_lane[-1], is_top)}
    end_row = {1: row == 0, -1: row == rows - 1}
    far_row = {1: rows - 1, -1: 0}
    side = {1: 0, -1: 1}

    def turn(v, c, axis):
        n = rows if axis == 0 else lanes
        return pltpu.roll(v, 1 if c == 1 else n - 1, axis)

    def plane(x):
        return pl.ds((x + 1) * rows, rows)

    def keep(s, x, out, packed):
        for q in range(POPS):
            post[s, POS[q], plane(x), :] = out[q]
        for cz in (1, -1):
            for j, q in enumerate(ZM[cz]):
                k = LANE0 + j * planes + x
                packed[cz] = jnp.where(lane == k, pltpu.roll(out[q], k + (1 if cz == 1 else 0), 1), packed[cz])

    def copy(s, m):
        kind, slot, off = MESSAGES[m]
        if kind == "x":
            some = pl.ds(0 if slot == 1 else FACE, FACE)
            src, dst = (planes - 1, -1) if slot == 1 else (0, planes)
            src, dst = post.at[s, some, plane(src)], post.at[s, some, plane(dst)]
        elif kind == "y":
            src, dst = ysend.at[s, side[slot]], yrecv.at[s, side[slot]]
        elif kind == "z":
            cz, cy = slot
            src, dst = zsend.at[s, side[cz]], zrecv.at[s, side[cz], cy + 1]
        else:
            src = post.at[s, POS[slot], plane(planes - 1 if off[0] == 1 else 0)]
            dst = ydiag.at[s, XY.index(slot)] if kind == "xy" else zdiag.at[s, XZ.index(slot)]
        return pltpu.make_async_remote_copy(
            src_ref=src,
            dst_ref=dst,
            send_sem=send_sem.at[s, m],
            recv_sem=recv_sem.at[s, m],
            device_id=at(off),
            device_id_type=MESH,
        )

    def of_kind(kinds, dz):
        return [m for m, (kind, _, off) in enumerate(MESSAGES) if kind in kinds and off[2] == dz]

    def each(s, kinds, act, up, down):
        for dz, when in ((1, up), (-1, down)):
            if of_kind(kinds, dz):

                @pl.when(when)
                def _():
                    for m in of_kind(kinds, dz):
                        act(copy(s, m))

        for m in of_kind(kinds, 0):
            act(copy(s, m))

    def start(s, kinds):
        each(s, kinds, lambda c: c.start(), jnp.logical_not(is_top), jnp.logical_not(is_bottom))

    def receive(s, kinds):
        each(s, kinds, lambda c: c.wait_recv(), jnp.logical_not(is_bottom), jnp.logical_not(is_top))

    def drain(s, kinds):
        each(s, kinds, lambda c: c.wait_send(), jnp.logical_not(is_top), jnp.logical_not(is_bottom))

    def pack(s, packed):
        for cy in (1, -1):
            first = rows + far_row[cy]
            for j, q in enumerate(YM[cy]):
                ysend[s, side[cy], j] = post[s, POS[q], pl.ds(first, planes, stride=rows), :]
        for cz in (1, -1):
            zsend[s, side[cz]] = packed[cz]

    def z_faces(s):
        tiles = {}
        for cz in (1, -1):
            own = zrecv[s, side[cz], 1]
            tiles[cz, 0] = own
            for cy in (1, -1):
                other = zrecv[s, side[cz], cy + 1]
                tiles[cz, cy] = turn(jnp.where(row == far_row[cy], other, own), cy, 0)
        return tiles

    def stream(s, x, tiles):
        f = {}
        for q in range(POPS):
            cx, cy, cz = LATTICE[q]
            v = post[s, POS[q], plane(x - cx), :]
            inside = 0 <= x - cx < planes
            if cy:
                if inside:
                    edge = yrecv[s, side[cy], YM[cy].index(q), pl.ds(x - cx, 1), :]
                else:
                    edge = ydiag[s, XY.index(q), pl.ds(far_row[cy], 1), :]
                v = jnp.where(end_row[cy], jnp.broadcast_to(edge, (rows, lanes)), turn(v, cy, 0))
            if cz:
                if inside:
                    k = LANE0 + ZM[cz].index(q) * planes + x - cx
                    edge = pltpu.roll(tiles[cz, cy], (lanes if cz == 1 else lanes - 1) - k, 1)
                else:
                    edge = turn(zdiag[s, XZ.index(q)], cz, 1)
                back = post[s, POS[opposite(q)], plane(x), :]
                if q >= FLOWS:
                    back = 0.25 * (HOT_WALL if cz == 1 else COLD_WALL) - back
                v = jnp.where(wall[cz], back, jnp.where(end_lane[cz], edge, turn(v, cz, 1)))
            f[q] = v
        return f

    blank = jnp.zeros((rows, lanes), jnp.float32)

    def first(x, packed):
        keep(0, x, collide({q: held[q, pl.ds(x * rows, rows), :] for q in range(POPS)}), packed)

    packed = {1: blank, -1: blank}
    for c in loads[:4]:
        c.wait()
    for x in ends:
        first(x, packed)
    pl.semaphore_wait(barrier, len(offsets) + roots - is_root.astype(jnp.int32))
    start(0, END_PLANES)
    for c in loads[4:]:
        c.wait()
    for x in inner:
        first(x, packed)
    pack(0, packed)
    start(0, ALL_PLANES)

    for s in range(1, STEPS):
        packed = {1: blank, -1: blank}
        receive(s - 1, ALL_PLANES)
        tiles = z_faces(s - 1)
        for x in inner:
            keep(s, x, collide(stream(s - 1, x, tiles)), packed)
        receive(s - 1, END_PLANES)
        for x in ends:
            keep(s, x, collide(stream(s - 1, x, tiles)), packed)
        start(s, END_PLANES)
        pack(s, packed)
        start(s, ALL_PLANES)

    def last(x, tiles):
        f = stream(STEPS - 1, x, tiles)
        for q in range(FLOWS):
            flow_out[q, pl.ds(x * rows, rows), :] = f[q]
        for q in range(FLOWS, POPS):
            heat_out[q - FLOWS, pl.ds(x * rows, rows), :] = f[q]
        return flux(f)

    receive(STEPS - 1, ALL_PLANES)
    tiles = z_faces(STEPS - 1)
    acc = blank
    for x in inner:
        acc = acc + last(x, tiles)
    receive(STEPS - 1, END_PLANES)
    for x in ends:
        acc = acc + last(x, tiles)

    mine = jnp.sum(acc, axis=0, keepdims=True)
    part[0] = mine
    parts[my_index] = mine
    base = lax.rem(my_index, roots)

    def to_root(d, k):
        return pltpu.make_async_remote_copy(
            src_ref=part.at[0],
            dst_ref=parts.at[my_index],
            send_sem=part_send.at[k],
            recv_sem=part_recv.at[0],
            device_id=lax.rem(base + d, roots),
            device_id_type=pl.DeviceIdType.LOGICAL,
        )

    for d in range(1, roots):
        to_root(d, 0).start()

    @pl.when(jnp.logical_not(is_root))
    def _():
        to_root(0, 1).start()

    half = nx // 2
    served = [me[0] + half, half - 1 - me[0], nx - 1 - me[0]]

    def to_served(i):
        return pltpu.make_async_remote_copy(
            src_ref=total.at[0],
            dst_ref=total.at[0],
            send_sem=total_send.at[i],
            recv_sem=total_recv.at[0],
            device_id=(served[i], me[1], me[2]),
            device_id_type=MESH,
        )

    def whole(n, k):
        some = parts.at[pl.ds(0, n)]
        return pltpu.make_async_remote_copy(
            src_ref=some,
            dst_ref=some,
            send_sem=part_send.at[k],
            recv_sem=part_recv.at[0],
            device_id=0,
            device_id_type=pl.DeviceIdType.LOGICAL,
        )

    @pl.when(is_root)
    def _():
        whole(count - 1, 0).wait_recv()
        sums = [parts[i] for i in range(8)]
        for i in range(8, count):
            sums[i % 8] = sums[i % 8] + parts[i]
        total[0] = ((sums[0] + sums[1]) + (sums[2] + sums[3])) + ((sums[4] + sums[5]) + (sums[6] + sums[7]))
        for i in range(3):
            to_served(i).start()

    @pl.when(jnp.logical_not(is_root))
    def _():
        to_served(0).wait_recv()

    cells = count * planes * rows * lanes
    scale = nz * lanes / (DIFFUSIVITY * (HOT_WALL - COLD_WALL)) / cells
    nusselt[0, 0] = 1.0 + scale * jnp.sum(total[0])

    whole(roots - 1, 0).wait_send()

    @pl.when(jnp.logical_not(is_root))
    def _():
        to_root(0, 1).wait_send()

    @pl.when(is_root)
    def _():
        for i in range(3):
            to_served(i).wait_send()

    for s in range(STEPS):
        drain(s, END_PLANES + ALL_PLANES)


def per_device(shape, flow_pops, heat_pops):
    nx, ny, nz = shape
    _, planes, rows, lanes = flow_pops.shape
    flat = (planes * rows, lanes)
    dma = pltpu.SemaphoreType.DMA
    tile = (rows, lanes)
    vmem = lambda *dims: pltpu.VMEM(dims, jnp.float32)
    anywhere = pl.BlockSpec(memory_space=pl.ANY)
    in_vmem = pl.BlockSpec(memory_space=pltpu.VMEM)
    flow, heat, nusselt = pl.pallas_call(
        functools.partial(kernel, shape, (planes, rows, lanes)),
        out_shape=(
            vmem(FLOWS, *flat),
            vmem(7, *flat),
            jax.ShapeDtypeStruct((1, 1), jnp.float32),
        ),
        in_specs=[anywhere] * 2,
        out_specs=(in_vmem, in_vmem, pl.BlockSpec(memory_space=pltpu.SMEM)),
        scratch_shapes=[
            vmem(POPS, *flat),
            vmem(STEPS, POPS, (planes + 2) * rows, lanes),
            vmem(STEPS, 2, FACE, *tile),
            vmem(STEPS, 2, FACE, *tile),
            vmem(STEPS, len(XY), *tile),
            vmem(STEPS, 2, *tile),
            vmem(STEPS, 2, 3, *tile),
            vmem(STEPS, len(XZ), *tile),
            vmem(1, 1, lanes),
            vmem(nx * ny * nz, 1, lanes),
            vmem(1, 1, lanes),
            dma((6,)),
            dma((STEPS, len(MESSAGES))),
            dma((STEPS, len(MESSAGES))),
            dma((2,)),
            dma((1,)),
            dma((3,)),
            dma((1,)),
        ],
        compiler_params=pltpu.CompilerParams(collective_id=0, has_side_effects=True),
        name="lattice_steps",
    )(flow_pops.reshape((FLOWS,) + flat), heat_pops.reshape((7,) + flat))
    return flow.reshape(flow_pops.shape), heat.reshape(heat_pops.shape), nusselt.reshape(())


def solution(mesh):
    shape = tuple(mesh.shape[a] for a in AXES)
    spec = P(None, *AXES)
    return jax.shard_map(
        functools.partial(per_device, shape),
        mesh=mesh,
        in_specs=(spec, spec),
        out_specs=(spec, spec, P()),
        check_vma=False,
    )
```

```python
import functools

import jax
import jax.numpy as jnp
import numpy as np
from jax import lax
from jax.experimental import pallas as pl
from jax.experimental.pallas import tpu as pltpu
from jax.sharding import PartitionSpec as P

MESH = pl.DeviceIdType.MESH
STEPS = 3
AXES = ("gx", "gy", "gz")

FLOW_SET = [
    (0, 0, 0),
    (1, 0, 0),
    (-1, 0, 0),
    (0, 1, 0),
    (0, -1, 0),
    (0, 0, 1),
    (0, 0, -1),
    (1, 1, 0),
    (-1, -1, 0),
    (1, -1, 0),
    (-1, 1, 0),
    (1, 0, 1),
    (-1, 0, -1),
    (1, 0, -1),
    (-1, 0, 1),
    (0, 1, 1),
    (0, -1, -1),
    (0, 1, -1),
    (0, -1, 1),
]
LATTICE = FLOW_SET + FLOW_SET[:7]
FLOWS = len(FLOW_SET)
POPS = len(LATTICE)
TAU_FLOW = 0.6
TAU_HEAT = 0.7
GRAVITY_LIFT = 0.01
HOT_WALL = 0.5
COLD_WALL = -0.5
DIFFUSIVITY = (TAU_HEAT - 0.5) / 4.0


def opposite(q):
    c = tuple(-v for v in LATTICE[q])
    return FLOW_SET.index(c) + (FLOWS if q >= FLOWS else 0)


def movers(axis, sign):
    return [q for q in range(POPS) if LATTICE[q][axis] == sign]


XP, XM = movers(0, 1), movers(0, -1)
YM = {1: movers(1, 1), -1: movers(1, -1)}
ZM = {1: movers(2, 1), -1: movers(2, -1)}
FACE = len(XP)
ORDER = XP + XM + [q for q in range(POPS) if LATTICE[q][0] == 0]
POS = {q: i for i, q in enumerate(ORDER)}
XY = [q for q in range(FLOWS) if LATTICE[q][0] != 0 and LATTICE[q][1] != 0]
XZ = [q for q in range(FLOWS) if LATTICE[q][0] != 0 and LATTICE[q][2] != 0]
LANE0 = 8


def messages():
    out = [("x", 1, (1, 0, 0)), ("x", -1, (-1, 0, 0))]
    out += [("xz", q, LATTICE[q]) for q in XZ]
    out += [("xy", q, LATTICE[q]) for q in XY]
    out += [("z", (cz, cy), (0, cy, cz)) for cz in (1, -1) for cy in (1, -1, 0)]
    out += [("y", 1, (0, 1, 0)), ("y", -1, (0, -1, 0))]
    return out


MESSAGES = messages()
END_PLANES = ("x", "xy", "xz")
ALL_PLANES = ("y", "z")


def collide(f):
    s, d = {}, {}
    for q in range(1, FLOWS, 2):
        s[q] = f[q] + f[q + 1]
        d[q] = f[q] - f[q + 1]
    rho = (((s[1] + s[3]) + (s[5] + s[7])) + ((s[9] + s[11]) + (s[13] + s[15]))) + (s[17] + f[0])
    jx = (d[1] + d[7]) + (d[9] + d[11]) + d[13]
    jy = (d[3] + d[7]) + (d[15] + d[17]) - d[9]
    jz = (d[5] + d[11]) + (d[15] - d[13]) - d[17]
    g = [f[FLOWS + i] for i in range(7)]
    warmth = ((g[0] + g[1]) + (g[2] + g[3])) + ((g[4] + g[5]) + g[6])
    force = GRAVITY_LIFT * rho * warmth
    inv = 1.0 / rho
    ux = jx * inv
    uy = jy * inv
    uz = (jz + 0.5 * force) * inv

    w2 = 1.0 / 36.0
    keep = 1.0 - 1.0 / TAU_FLOW
    r = (w2 / TAU_FLOW) * rho
    sf = (w2 * (1.0 - 0.5 / TAU_FLOW)) * force
    r3 = 3.0 * r
    rx, ry, rz = r3 * ux, r3 * uy, r3 * uz
    sf3 = 3.0 * sf
    ax, ay, az = rx, ry, rz + sf3
    bx, by, bz = 1.5 * rx, 1.5 * ry, 1.5 * rz + 3.0 * sf3
    qx, qy, qz = ux * bx, uy * by, uz * bz
    usq = rx * ux + ry * uy + rz * uz
    base = r - 0.5 * usq - sf3 * uz
    cxy = ux * by + uy * bx
    cxz = ux * bz + uz * bx
    cyz = uy * bz + uz * by

    out = {0: keep * f[0] + 12.0 * base}

    def pair(q, even, odd):
        out[q] = keep * f[q] + (even + odd)
        out[q + 1] = keep * f[q + 1] + (even - odd)

    pair(1, 2.0 * (base + qx), 2.0 * ax)
    pair(3, 2.0 * (base + qy), 2.0 * ay)
    pair(5, 2.0 * (base + qz), 2.0 * az)
    exy = base + (qx + qy)
    exz = base + (qx + qz)
    eyz = base + (qy + qz)
    pair(7, exy + cxy, ax + ay)
    pair(9, exy - cxy, ax - ay)
    pair(11, exz + cxz, ax + az)
    pair(13, exz - cxz, ax - az)
    pair(15, eyz + cyz, ay + az)
    pair(17, eyz - cyz, ay - az)

    keep_heat = 1.0 - 1.0 / TAU_HEAT
    t8 = (0.125 / TAU_HEAT) * warmth
    t2 = 4.0 * t8
    out[FLOWS] = keep_heat * g[0] + 2.0 * t8
    for i, u in ((1, ux), (3, uy), (5, uz)):
        odd = t2 * u
        out[FLOWS + i] = keep_heat * g[i] + (t8 + odd)
        out[FLOWS + i + 1] = keep_heat * g[i + 1] + (t8 - odd)
    return out


def flux(f):
    total = lambda values: functools.reduce(lambda a, b: a + b, values)
    rho = total([f[q] for q in range(FLOWS)])
    jz = total([f[q] for q in range(FLOWS) if LATTICE[q][2] == 1]) - total(
        [f[q] for q in range(FLOWS) if LATTICE[q][2] == -1]
    )
    warmth = total([f[q] for q in range(FLOWS, POPS)])
    force = GRAVITY_LIFT * rho * warmth
    return (jz + 0.5 * force) / rho * warmth


def kernel(
    shape,
    sizes,
    flow_in,
    heat_in,
    flow_out,
    heat_out,
    nusselt,
    held,
    post,
    ysend,
    yrecv,
    ydiag,
    zsend,
    zrecv,
    zdiag,
    part,
    parts,
    total,
    in_sem,
    send_sem,
    recv_sem,
    part_send,
    part_recv,
    total_send,
    total_recv,
):
    nx, ny, nz = shape
    planes, rows, lanes = sizes
    me = tuple(lax.axis_index(a) for a in AXES)
    count = nx * ny * nz
    group = ny * nz
    roots = (nx // 4) * group
    my_index = me[0] * group + me[1] * nz + me[2]
    is_root = me[0] < nx // 4

    def at(off):
        return tuple(m if d == 0 else lax.rem(m + (d % n), n) for m, d, n in zip(me, off, shape))

    offsets = [off for off in np.ndindex(3, 3, 3) if off != (1, 1, 1)]
    offsets = [tuple(d - 1 for d in off) for off in offsets if 1 in off]
    barrier = pltpu.get_barrier_semaphore()
    for off in offsets:
        pl.semaphore_signal(barrier, inc=1, device_id=at(off), device_id_type=MESH)

    inner, ends = range(1, planes - 1), (0, planes - 1)
    blocks = [(0, 1), (planes - 1, 1), (1, planes - 2)]
    loads = []
    for i, (x, n) in enumerate(blocks):
        some = pl.ds(x * rows, n * rows)
        for j, (ref, low, n) in enumerate(((flow_in, 0, FLOWS), (heat_in, FLOWS, 7))):
            loads.append(
                pltpu.make_async_copy(ref.at[:, some], held.at[pl.ds(low, n), some], in_sem.at[2 * i + j])
            )
    for c in loads:
        c.start()

    @pl.when(is_root)
    def _():
        for d in range(1, nx):
            pl.semaphore_signal(barrier, inc=1, device_id=at((d, 0, 0)), device_id_type=MESH)

    lane = lax.broadcasted_iota(jnp.int32, (rows, lanes), 1)
    row = lax.broadcasted_iota(jnp.int32, (rows, lanes), 0)
    is_bottom = me[2] == 0
    is_top = me[2] == nz - 1
    end_lane = {1: lane == 0, -1: lane == lanes - 1}
    wall = {1: jnp.logical_and(end_lane[1], is_bottom), -1: jnp.logical_and(end_lane[-1], is_top)}
    end_row = {1: row == 0, -1: row == rows - 1}
    far_row = {1: rows - 1, -1: 0}
    side = {1: 0, -1: 1}

    def turn(v, c, axis):
        n = rows if axis == 0 else lanes
        return pltpu.roll(v, 1 if c == 1 else n - 1, axis)

    def plane(x):
        return pl.ds((x + 1) * rows, rows)

    def keep(s, x, out, packed):
        for q in range(POPS):
            post[s, POS[q], plane(x), :] = out[q]
        for cz in (1, -1):
            for j, q in enumerate(ZM[cz]):
                k = LANE0 + j * planes + x
                packed[cz] = jnp.where(lane == k, pltpu.roll(out[q], k + (1 if cz == 1 else 0), 1), packed[cz])

    def copy(s, m):
        kind, slot, off = MESSAGES[m]
        if kind == "x":
            some = pl.ds(0 if slot == 1 else FACE, FACE)
            src, dst = (planes - 1, -1) if slot == 1 else (0, planes)
            src, dst = post.at[s, some, plane(src)], post.at[s, some, plane(dst)]
        elif kind == "y":
            src, dst = ysend.at[s, side[slot]], yrecv.at[s, side[slot]]
        elif kind == "z":
            cz, cy = slot
            src, dst = zsend.at[s, side[cz]], zrecv.at[s, side[cz], cy + 1]
        else:
            src = post.at[s, POS[slot], plane(planes - 1 if off[0] == 1 else 0)]
            dst = ydiag.at[s, XY.index(slot)] if kind == "xy" else zdiag.at[s, XZ.index(slot)]
        return pltpu.make_async_remote_copy(
            src_ref=src,
            dst_ref=dst,
            send_sem=send_sem.at[s, m],
            recv_sem=recv_sem.at[s, m],
            device_id=at(off),
            device_id_type=MESH,
        )

    def of_kind(kinds, dz):
        return [m for m, (kind, _, off) in enumerate(MESSAGES) if kind in kinds and off[2] == dz]

    def each(s, kinds, act, up, down):
        for dz, when in ((1, up), (-1, down)):
            if of_kind(kinds, dz):

                @pl.when(when)
                def _():
                    for m in of_kind(kinds, dz):
                        act(copy(s, m))

        for m in of_kind(kinds, 0):
            act(copy(s, m))

    def start(s, kinds):
        each(s, kinds, lambda c: c.start(), jnp.logical_not(is_top), jnp.logical_not(is_bottom))

    def receive(s, kinds):
        each(s, kinds, lambda c: c.wait_recv(), jnp.logical_not(is_bottom), jnp.logical_not(is_top))

    def drain(s, kinds):
        each(s, kinds, lambda c: c.wait_send(), jnp.logical_not(is_top), jnp.logical_not(is_bottom))

    def pack(s, packed):
        for cy in (1, -1):
            first = rows + far_row[cy]
            for j, q in enumerate(YM[cy]):
                ysend[s, side[cy], j] = post[s, POS[q], pl.ds(first, planes, stride=rows), :]
        for cz in (1, -1):
            zsend[s, side[cz]] = packed[cz]

    def z_faces(s):
        tiles = {}
        for cz in (1, -1):
            own = zrecv[s, side[cz], 1]
            tiles[cz, 0] = own
            for cy in (1, -1):
                other = zrecv[s, side[cz], cy + 1]
                tiles[cz, cy] = turn(jnp.where(row == far_row[cy], other, own), cy, 0)
        return tiles

    def stream(s, x, tiles):
        f = {}
        for q in range(POPS):
            cx, cy, cz = LATTICE[q]
            v = post[s, POS[q], plane(x - cx), :]
            inside = 0 <= x - cx < planes
            if cy:
                if inside:
                    edge = yrecv[s, side[cy], YM[cy].index(q), pl.ds(x - cx, 1), :]
                else:
                    edge = ydiag[s, XY.index(q), pl.ds(far_row[cy], 1), :]
                v = jnp.where(end_row[cy], jnp.broadcast_to(edge, (rows, lanes)), turn(v, cy, 0))
            if cz:
                if inside:
                    k = LANE0 + ZM[cz].index(q) * planes + x - cx
                    edge = pltpu.roll(tiles[cz, cy], (lanes if cz == 1 else lanes - 1) - k, 1)
                else:
                    edge = turn(zdiag[s, XZ.index(q)], cz, 1)
                back = post[s, POS[opposite(q)], plane(x), :]
                if q >= FLOWS:
                    back = 0.25 * (HOT_WALL if cz == 1 else COLD_WALL) - back
                v = jnp.where(wall[cz], back, jnp.where(end_lane[cz], edge, turn(v, cz, 1)))
            f[q] = v
        return f

    blank = jnp.zeros((rows, lanes), jnp.float32)

    def first(x, packed):
        keep(0, x, collide({q: held[q, pl.ds(x * rows, rows), :] for q in range(POPS)}), packed)

    packed = {1: blank, -1: blank}
    for c in loads[:4]:
        c.wait()
    for x in ends:
        first(x, packed)
    pl.semaphore_wait(barrier, len(offsets) + nx // 4 - is_root.astype(jnp.int32))
    start(0, END_PLANES)
    for c in loads[4:]:
        c.wait()
    for x in inner:
        first(x, packed)
    pack(0, packed)
    start(0, ALL_PLANES)

    for s in range(1, STEPS):
        packed = {1: blank, -1: blank}
        receive(s - 1, ALL_PLANES)
        tiles = z_faces(s - 1)
        for x in inner:
            keep(s, x, collide(stream(s - 1, x, tiles)), packed)
        receive(s - 1, END_PLANES)
        for x in ends:
            keep(s, x, collide(stream(s - 1, x, tiles)), packed)
        start(s, END_PLANES)
        pack(s, packed)
        start(s, ALL_PLANES)

    def last(x, tiles):
        f = stream(STEPS - 1, x, tiles)
        for q in range(FLOWS):
            flow_out[q, pl.ds(x * rows, rows), :] = f[q]
        for q in range(FLOWS, POPS):
            heat_out[q - FLOWS, pl.ds(x * rows, rows), :] = f[q]
        return flux(f)

    receive(STEPS - 1, ALL_PLANES)
    tiles = z_faces(STEPS - 1)
    acc = blank
    for x in inner:
        acc = acc + last(x, tiles)
    receive(STEPS - 1, END_PLANES)
    for x in ends:
        acc = acc + last(x, tiles)

    mine = jnp.sum(acc, axis=0, keepdims=True)
    part[0] = mine
    parts[my_index] = mine
    base = lax.rem(my_index, roots)

    def to_root(d, k):
        return pltpu.make_async_remote_copy(
            src_ref=part.at[0],
            dst_ref=parts.at[my_index],
            send_sem=part_send.at[k],
            recv_sem=part_recv.at[0],
            device_id=lax.rem(base + d, roots),
            device_id_type=pl.DeviceIdType.LOGICAL,
        )

    for d in range(1, roots):
        to_root(d, 0).start()

    @pl.when(jnp.logical_not(is_root))
    def _():
        to_root(0, 1).start()

    half = nx // 2
    served = [me[0] + half, half - 1 - me[0], nx - 1 - me[0]]

    def to_served(i):
        return pltpu.make_async_remote_copy(
            src_ref=total.at[0],
            dst_ref=total.at[0],
            send_sem=total_send.at[i],
            recv_sem=total_recv.at[0],
            device_id=(served[i], me[1], me[2]),
            device_id_type=MESH,
        )

    def whole(n, k):
        some = parts.at[pl.ds(0, n)]
        return pltpu.make_async_remote_copy(
            src_ref=some,
            dst_ref=some,
            send_sem=part_send.at[k],
            recv_sem=part_recv.at[0],
            device_id=0,
            device_id_type=pl.DeviceIdType.LOGICAL,
        )

    @pl.when(is_root)
    def _():
        whole(count - 1, 0).wait_recv()
        sums = [parts[i] for i in range(8)]
        for i in range(8, count):
            sums[i % 8] = sums[i % 8] + parts[i]
        total[0] = ((sums[0] + sums[1]) + (sums[2] + sums[3])) + ((sums[4] + sums[5]) + (sums[6] + sums[7]))
        for i in range(3):
            to_served(i).start()

    @pl.when(jnp.logical_not(is_root))
    def _():
        to_served(0).wait_recv()

    cells = count * planes * rows * lanes
    scale = nz * lanes / (DIFFUSIVITY * (HOT_WALL - COLD_WALL)) / cells
    nusselt[0, 0] = 1.0 + scale * jnp.sum(total[0])

    whole(roots - 1, 0).wait_send()

    @pl.when(jnp.logical_not(is_root))
    def _():
        to_root(0, 1).wait_send()

    @pl.when(is_root)
    def _():
        for i in range(3):
            to_served(i).wait_send()

    for s in range(STEPS):
        drain(s, END_PLANES + ALL_PLANES)


def write_out(flow, heat, flow_out, heat_out, sem):
    copies = [
        pltpu.make_async_copy(flow, flow_out, sem.at[0]),
        pltpu.make_async_copy(heat, heat_out, sem.at[1]),
    ]
    for c in copies:
        c.start()
    for c in copies:
        c.wait()


def per_device(shape, flow_pops, heat_pops):
    nx, ny, nz = shape
    _, planes, rows, lanes = flow_pops.shape
    flat = (planes * rows, lanes)
    dma = pltpu.SemaphoreType.DMA
    tile = (rows, lanes)
    vmem = lambda *dims: pltpu.VMEM(dims, jnp.float32)
    anywhere = pl.BlockSpec(memory_space=pl.ANY)
    in_vmem = pl.BlockSpec(memory_space=pltpu.VMEM)
    flow, heat, nusselt = pl.pallas_call(
        functools.partial(kernel, shape, (planes, rows, lanes)),
        out_shape=(
            vmem(FLOWS, *flat),
            vmem(7, *flat),
            jax.ShapeDtypeStruct((1, 1), jnp.float32),
        ),
        in_specs=[anywhere] * 2,
        out_specs=(in_vmem, in_vmem, pl.BlockSpec(memory_space=pltpu.SMEM)),
        scratch_shapes=[
            vmem(POPS, *flat),
            vmem(STEPS, POPS, (planes + 2) * rows, lanes),
            vmem(STEPS, 2, FACE, *tile),
            vmem(STEPS, 2, FACE, *tile),
            vmem(STEPS, len(XY), *tile),
            vmem(STEPS, 2, *tile),
            vmem(STEPS, 2, 3, *tile),
            vmem(STEPS, len(XZ), *tile),
            vmem(1, 1, lanes),
            vmem(nx * ny * nz, 1, lanes),
            vmem(1, 1, lanes),
            dma((6,)),
            dma((STEPS, len(MESSAGES))),
            dma((STEPS, len(MESSAGES))),
            dma((2,)),
            dma((1,)),
            dma((3,)),
            dma((1,)),
        ],
        compiler_params=pltpu.CompilerParams(collective_id=0, has_side_effects=True),
        name="lattice_steps",
    )(flow_pops.reshape((FLOWS,) + flat), heat_pops.reshape((7,) + flat))
    flow = pltpu.with_memory_space_constraint(flow, pltpu.VMEM)
    heat = pltpu.with_memory_space_constraint(heat, pltpu.VMEM)
    flow, heat = pl.pallas_call(
        write_out,
        out_shape=(jax.ShapeDtypeStruct((FLOWS,) + flat, jnp.float32), jax.ShapeDtypeStruct((7,) + flat, jnp.float32)),
        in_specs=[in_vmem] * 2,
        out_specs=(anywhere, anywhere),
        scratch_shapes=[dma((2,))],
        name="write_out",
    )(flow, heat)
    return flow.reshape(flow_pops.shape), heat.reshape(heat_pops.shape), nusselt.reshape(())


def solution(mesh):
    shape = tuple(mesh.shape[a] for a in AXES)
    spec = P(None, *AXES)
    return jax.shard_map(
        functools.partial(per_device, shape),
        mesh=mesh,
        in_specs=(spec, spec),
        out_specs=(spec, spec, P()),
        check_vma=False,
    )
```

```python
import functools

import jax
import jax.numpy as jnp
import numpy as np
from jax import lax
from jax.experimental import pallas as pl
from jax.experimental.pallas import tpu as pltpu
from jax.sharding import PartitionSpec as P

MESH = pl.DeviceIdType.MESH
STEPS = 3
AXES = ("gx", "gy", "gz")

FLOW_SET = [
    (0, 0, 0),
    (1, 0, 0),
    (-1, 0, 0),
    (0, 1, 0),
    (0, -1, 0),
    (0, 0, 1),
    (0, 0, -1),
    (1, 1, 0),
    (-1, -1, 0),
    (1, -1, 0),
    (-1, 1, 0),
    (1, 0, 1),
    (-1, 0, -1),
    (1, 0, -1),
    (-1, 0, 1),
    (0, 1, 1),
    (0, -1, -1),
    (0, 1, -1),
    (0, -1, 1),
]
LATTICE = FLOW_SET + FLOW_SET[:7]
FLOWS = len(FLOW_SET)
POPS = len(LATTICE)
TAU_FLOW = 0.6
TAU_HEAT = 0.7
GRAVITY_LIFT = 0.01
HOT_WALL = 0.5
COLD_WALL = -0.5
DIFFUSIVITY = (TAU_HEAT - 0.5) / 4.0


def opposite(q):
    c = tuple(-v for v in LATTICE[q])
    return FLOW_SET.index(c) + (FLOWS if q >= FLOWS else 0)


def movers(axis, sign):
    return [q for q in range(POPS) if LATTICE[q][axis] == sign]


XP, XM = movers(0, 1), movers(0, -1)
YM = {1: movers(1, 1), -1: movers(1, -1)}
ZM = {1: movers(2, 1), -1: movers(2, -1)}
FACE = len(XP)
ORDER = XP + XM + [q for q in range(POPS) if LATTICE[q][0] == 0]
POS = {q: i for i, q in enumerate(ORDER)}
XY = [q for q in range(FLOWS) if LATTICE[q][0] != 0 and LATTICE[q][1] != 0]
XZ = [q for q in range(FLOWS) if LATTICE[q][0] != 0 and LATTICE[q][2] != 0]
LANE0 = 8


def messages():
    out = [("x", 1, (1, 0, 0)), ("x", -1, (-1, 0, 0))]
    out += [("xz", q, LATTICE[q]) for q in XZ]
    out += [("xy", q, LATTICE[q]) for q in XY]
    out += [("yz", (cz, cy), (0, cy, cz)) for cz in (1, -1) for cy in (1, -1)]
    out += [("z", cz, (0, 0, cz)) for cz in (1, -1)]
    out += [("y", 1, (0, 1, 0)), ("y", -1, (0, -1, 0))]
    return out


MESSAGES = messages()
EDGE = {m[:2]: i for i, m in enumerate(m for m in MESSAGES if m[0] in ("xy", "yz"))}
END_PLANES = ("x", "xy", "xz")
ALL_PLANES = ("y", "z", "yz")


def collide(f):
    s, d = {}, {}
    for q in range(1, FLOWS, 2):
        s[q] = f[q] + f[q + 1]
        d[q] = f[q] - f[q + 1]
    rho = (((s[1] + s[3]) + (s[5] + s[7])) + ((s[9] + s[11]) + (s[13] + s[15]))) + (s[17] + f[0])
    jx = (d[1] + d[7]) + (d[9] + d[11]) + d[13]
    jy = (d[3] + d[7]) + (d[15] + d[17]) - d[9]
    jz = (d[5] + d[11]) + (d[15] - d[13]) - d[17]
    g = [f[FLOWS + i] for i in range(7)]
    warmth = ((g[0] + g[1]) + (g[2] + g[3])) + ((g[4] + g[5]) + g[6])
    force = GRAVITY_LIFT * rho * warmth
    inv = 1.0 / rho
    ux = jx * inv
    uy = jy * inv
    uz = (jz + 0.5 * force) * inv

    w2 = 1.0 / 36.0
    keep = 1.0 - 1.0 / TAU_FLOW
    r = (w2 / TAU_FLOW) * rho
    sf = (w2 * (1.0 - 0.5 / TAU_FLOW)) * force
    r3 = 3.0 * r
    rx, ry, rz = r3 * ux, r3 * uy, r3 * uz
    sf3 = 3.0 * sf
    ax, ay, az = rx, ry, rz + sf3
    bx, by, bz = 1.5 * rx, 1.5 * ry, 1.5 * rz + 3.0 * sf3
    qx, qy, qz = ux * bx, uy * by, uz * bz
    usq = rx * ux + ry * uy + rz * uz
    base = r - 0.5 * usq - sf3 * uz
    cxy = ux * by + uy * bx
    cxz = ux * bz + uz * bx
    cyz = uy * bz + uz * by

    out = {0: keep * f[0] + 12.0 * base}

    def pair(q, even, odd):
        out[q] = keep * f[q] + (even + odd)
        out[q + 1] = keep * f[q + 1] + (even - odd)

    pair(1, 2.0 * (base + qx), 2.0 * ax)
    pair(3, 2.0 * (base + qy), 2.0 * ay)
    pair(5, 2.0 * (base + qz), 2.0 * az)
    exy = base + (qx + qy)
    exz = base + (qx + qz)
    eyz = base + (qy + qz)
    pair(7, exy + cxy, ax + ay)
    pair(9, exy - cxy, ax - ay)
    pair(11, exz + cxz, ax + az)
    pair(13, exz - cxz, ax - az)
    pair(15, eyz + cyz, ay + az)
    pair(17, eyz - cyz, ay - az)

    keep_heat = 1.0 - 1.0 / TAU_HEAT
    t8 = (0.125 / TAU_HEAT) * warmth
    t2 = 4.0 * t8
    out[FLOWS] = keep_heat * g[0] + 2.0 * t8
    for i, u in ((1, ux), (3, uy), (5, uz)):
        odd = t2 * u
        out[FLOWS + i] = keep_heat * g[i] + (t8 + odd)
        out[FLOWS + i + 1] = keep_heat * g[i + 1] + (t8 - odd)
    return out


def flux(f):
    total = lambda values: functools.reduce(lambda a, b: a + b, values)
    rho = total([f[q] for q in range(FLOWS)])
    jz = total([f[q] for q in range(FLOWS) if LATTICE[q][2] == 1]) - total(
        [f[q] for q in range(FLOWS) if LATTICE[q][2] == -1]
    )
    warmth = total([f[q] for q in range(FLOWS, POPS)])
    force = GRAVITY_LIFT * rho * warmth
    return (jz + 0.5 * force) / rho * warmth


def kernel(
    shape,
    sizes,
    flow_in,
    heat_in,
    flow_out,
    heat_out,
    total,
    held,
    post,
    ysend,
    yrecv,
    zsend,
    zrecv,
    zdiag,
    edge_send,
    edge_recv,
    part,
    parts,
    in_sem,
    send_sem,
    recv_sem,
    part_send,
    part_recv,
    total_send,
    total_recv,
):
    nx, ny, nz = shape
    planes, rows, lanes = sizes
    me = tuple(lax.axis_index(a) for a in AXES)
    count = nx * ny * nz
    group = ny * nz
    my_index = me[0] * group + me[1] * nz + me[2]
    is_root = lax.rem(me[0], nx // 2) < nx // 4

    def at(off):
        return tuple(m if d == 0 else lax.rem(m + (d % n), n) for m, d, n in zip(me, off, shape))

    offsets = [off for off in np.ndindex(3, 3, 3) if off != (1, 1, 1)]
    offsets = [tuple(d - 1 for d in off) for off in offsets if 1 in off]
    barrier = pltpu.get_barrier_semaphore()
    for off in offsets:
        pl.semaphore_signal(barrier, inc=1, device_id=at(off), device_id_type=MESH)

    inner, ends = range(1, planes - 1), (0, planes - 1)
    blocks = [(0, 1), (planes - 1, 1), (1, planes - 2)]
    loads = []
    for i, (x, n) in enumerate(blocks):
        some = pl.ds(x * rows, n * rows)
        for j, (ref, low, n) in enumerate(((flow_in, 0, FLOWS), (heat_in, FLOWS, 7))):
            loads.append(
                pltpu.make_async_copy(ref.at[:, some], held.at[pl.ds(low, n), some], in_sem.at[2 * i + j])
            )
    for c in loads:
        c.start()

    @pl.when(is_root)
    def _():
        for d in range(1, nx):
            pl.semaphore_signal(barrier, inc=1, device_id=at((d, 0, 0)), device_id_type=MESH)

    lane = lax.broadcasted_iota(jnp.int32, (rows, lanes), 1)
    row = lax.broadcasted_iota(jnp.int32, (rows, lanes), 0)
    is_bottom = me[2] == 0
    is_top = me[2] == nz - 1
    end_lane = {1: lane == 0, -1: lane == lanes - 1}
    wall = {1: jnp.logical_and(end_lane[1], is_bottom), -1: jnp.logical_and(end_lane[-1], is_top)}
    end_row = {1: row == 0, -1: row == rows - 1}
    far_row = {1: rows - 1, -1: 0}
    side = {1: 0, -1: 1}

    def turn(v, c, axis):
        n = rows if axis == 0 else lanes
        return pltpu.roll(v, 1 if c == 1 else n - 1, axis)

    def plane(x):
        return pl.ds((x + 1) * rows, rows)

    def keep(s, x, out, packed):
        if x in ends:
            cx = 1 if x else -1
            for q in XY:
                if LATTICE[q][0] == cx:
                    far = far_row[LATTICE[q][1]]
                    edge_send[s, EDGE["xy", q]] = out[q][far : far + 1, :]
        for q in range(POPS):
            post[s, POS[q], plane(x), :] = out[q]
        for cz in (1, -1):
            for j, q in enumerate(ZM[cz]):
                k = LANE0 + j * planes + x
                packed[cz] = jnp.where(lane == k, pltpu.roll(out[q], k + (1 if cz == 1 else 0), 1), packed[cz])

    def copy(s, m):
        kind, slot, off = MESSAGES[m]
        if kind == "x":
            some = pl.ds(0 if slot == 1 else FACE, FACE)
            src, dst = (planes - 1, -1) if slot == 1 else (0, planes)
            src, dst = post.at[s, some, plane(src)], post.at[s, some, plane(dst)]
        elif kind == "y":
            src, dst = ysend.at[s, side[slot]], yrecv.at[s, side[slot]]
        elif kind == "z":
            src, dst = zsend.at[s, side[slot]], zrecv.at[s, side[slot]]
        elif kind == "xz":
            src = post.at[s, POS[slot], plane(planes - 1 if off[0] == 1 else 0)]
            dst = zdiag.at[s, XZ.index(slot)]
        else:
            src, dst = edge_send.at[s, EDGE[kind, slot]], edge_recv.at[s, EDGE[kind, slot]]
        return pltpu.make_async_remote_copy(
            src_ref=src,
            dst_ref=dst,
            send_sem=send_sem.at[s, m],
            recv_sem=recv_sem.at[s, m],
            device_id=at(off),
            device_id_type=MESH,
        )

    def of_kind(kinds, dz):
        return [m for m, (kind, _, off) in enumerate(MESSAGES) if kind in kinds and off[2] == dz]

    def each(s, kinds, act, up, down):
        for dz, when in ((1, up), (-1, down)):
            if of_kind(kinds, dz):

                @pl.when(when)
                def _():
                    for m in of_kind(kinds, dz):
                        act(copy(s, m))

        for m in of_kind(kinds, 0):
            act(copy(s, m))

    def start(s, kinds):
        each(s, kinds, lambda c: c.start(), jnp.logical_not(is_top), jnp.logical_not(is_bottom))

    def receive(s, kinds):
        each(s, kinds, lambda c: c.wait_recv(), jnp.logical_not(is_bottom), jnp.logical_not(is_top))

    def drain(s, kinds):
        each(s, kinds, lambda c: c.wait_send(), jnp.logical_not(is_top), jnp.logical_not(is_bottom))

    def pack(s, packed):
        for cy in (1, -1):
            first = rows + far_row[cy]
            for j, q in enumerate(YM[cy]):
                ysend[s, side[cy], j] = post[s, POS[q], pl.ds(first, planes, stride=rows), :]
        for cz in (1, -1):
            zsend[s, side[cz]] = packed[cz]
            for cy in (1, -1):
                far = far_row[cy]
                edge_send[s, EDGE["yz", (cz, cy)]] = packed[cz][far : far + 1, :]

    def z_faces(s):
        tiles = {}
        for cz in (1, -1):
            own = zrecv[s, side[cz]]
            tiles[cz, 0] = own
            for cy in (1, -1):
                other = jnp.broadcast_to(edge_recv[s, EDGE["yz", (cz, cy)]], (rows, lanes))
                tiles[cz, cy] = jnp.where(end_row[cy], other, turn(own, cy, 0))
        return tiles

    def stream(s, x, tiles):
        f = {}
        for q in range(POPS):
            cx, cy, cz = LATTICE[q]
            v = post[s, POS[q], plane(x - cx), :]
            inside = 0 <= x - cx < planes
            if cy:
                if inside:
                    edge = yrecv[s, side[cy], YM[cy].index(q), pl.ds(x - cx, 1), :]
                else:
                    edge = edge_recv[s, EDGE["xy", q]]
                v = jnp.where(end_row[cy], jnp.broadcast_to(edge, (rows, lanes)), turn(v, cy, 0))
            if cz:
                if inside:
                    k = LANE0 + ZM[cz].index(q) * planes + x - cx
                    edge = pltpu.roll(tiles[cz, cy], (lanes if cz == 1 else lanes - 1) - k, 1)
                else:
                    edge = turn(zdiag[s, XZ.index(q)], cz, 1)
                back = post[s, POS[opposite(q)], plane(x), :]
                if q >= FLOWS:
                    back = 0.25 * (HOT_WALL if cz == 1 else COLD_WALL) - back
                v = jnp.where(wall[cz], back, jnp.where(end_lane[cz], edge, turn(v, cz, 1)))
            f[q] = v
        return f

    blank = jnp.zeros((rows, lanes), jnp.float32)

    def first(x, packed):
        keep(0, x, collide({q: held[q, pl.ds(x * rows, rows), :] for q in range(POPS)}), packed)

    packed = {1: blank, -1: blank}
    for c in loads[:4]:
        c.wait()
    for x in ends:
        first(x, packed)
    pl.semaphore_wait(barrier, len(offsets) + nx // 2 - is_root.astype(jnp.int32))
    start(0, END_PLANES)
    for c in loads[4:]:
        c.wait()
    for x in inner:
        first(x, packed)
    pack(0, packed)
    start(0, ALL_PLANES)

    for s in range(1, STEPS):
        packed = {1: blank, -1: blank}
        receive(s - 1, ALL_PLANES)
        tiles = z_faces(s - 1)
        for x in inner:
            keep(s, x, collide(stream(s - 1, x, tiles)), packed)
        receive(s - 1, END_PLANES)
        for x in ends:
            keep(s, x, collide(stream(s - 1, x, tiles)), packed)
        start(s, END_PLANES)
        pack(s, packed)
        start(s, ALL_PLANES)

    def last(x, tiles):
        f = stream(STEPS - 1, x, tiles)
        for q in range(FLOWS):
            flow_out[q, pl.ds(x * rows, rows), :] = f[q]
        for q in range(FLOWS, POPS):
            heat_out[q - FLOWS, pl.ds(x * rows, rows), :] = f[q]
        return flux(f)

    receive(STEPS - 1, ALL_PLANES)
    tiles = z_faces(STEPS - 1)
    acc = blank
    for x in inner:
        acc = acc + last(x, tiles)
    receive(STEPS - 1, END_PLANES)
    for x in ends:
        acc = acc + last(x, tiles)

    mine = jnp.sum(acc, axis=0, keepdims=True)
    part[0] = mine
    parts[my_index] = mine
    seat = lax.rem(my_index, group)
    half = nx // 2
    lines = [x for x in range(nx) if x % half < nx // 4]

    def to_root(x, d, sem):
        return pltpu.make_async_remote_copy(
            src_ref=part.at[0],
            dst_ref=parts.at[my_index],
            send_sem=part_send.at[sem],
            recv_sem=part_recv.at[0],
            device_id=x * group + lax.rem(seat + d, group),
            device_id_type=pl.DeviceIdType.LOGICAL,
        )

    def not_self(x, act):
        @pl.when(me[0] != x)
        def _():
            act(to_root(x, 0, 1 + lines.index(x)))

    for x in lines:
        not_self(x, lambda c: c.start())
        for d in range(1, group):
            to_root(x, d, 0).start()

    served = [half - 1 - lax.rem(me[0], half) + half * lax.div(me[0], half)]

    def to_served(i):
        return pltpu.make_async_remote_copy(
            src_ref=total.at[0],
            dst_ref=total.at[0],
            send_sem=total_send.at[i],
            recv_sem=total_recv.at[0],
            device_id=(served[i], me[1], me[2]),
            device_id_type=MESH,
        )

    def whole(n, k):
        some = parts.at[pl.ds(0, n)]
        return pltpu.make_async_remote_copy(
            src_ref=some,
            dst_ref=some,
            send_sem=part_send.at[k],
            recv_sem=part_recv.at[0],
            device_id=0,
            device_id_type=pl.DeviceIdType.LOGICAL,
        )

    @pl.when(is_root)
    def _():
        whole(count - 1, 0).wait_recv()
        sums = [parts[i] for i in range(8)]
        for i in range(8, count):
            sums[i % 8] = sums[i % 8] + parts[i]
        total[0] = ((sums[0] + sums[1]) + (sums[2] + sums[3])) + ((sums[4] + sums[5]) + (sums[6] + sums[7]))
        for i in range(1):
            to_served(i).start()

    @pl.when(jnp.logical_not(is_root))
    def _():
        to_served(0).wait_recv()

    whole(len(lines) * (group - 1), 0).wait_send()
    for x in lines:
        not_self(x, lambda c: c.wait_send())

    @pl.when(is_root)
    def _():
        for i in range(1):
            to_served(i).wait_send()

    for s in range(STEPS):
        drain(s, END_PLANES + ALL_PLANES)


def write_out(scale, flow, heat, total, flow_out, heat_out, nusselt, sem):
    copies = [
        pltpu.make_async_copy(flow, flow_out, sem.at[0]),
        pltpu.make_async_copy(heat, heat_out, sem.at[1]),
    ]
    for c in copies:
        c.start()
    nusselt[0, 0] = 1.0 + scale * jnp.sum(total[0])
    for c in copies:
        c.wait()


def per_device(shape, flow_pops, heat_pops):
    nx, ny, nz = shape
    _, planes, rows, lanes = flow_pops.shape
    flat = (planes * rows, lanes)
    dma = pltpu.SemaphoreType.DMA
    tile = (rows, lanes)
    vmem = lambda *dims: pltpu.VMEM(dims, jnp.float32)
    anywhere = pl.BlockSpec(memory_space=pl.ANY)
    in_vmem = pl.BlockSpec(memory_space=pltpu.VMEM)
    state = pl.pallas_call(
        functools.partial(kernel, shape, (planes, rows, lanes)),
        out_shape=(
            vmem(FLOWS, *flat),
            vmem(7, *flat),
            vmem(1, 1, lanes),
        ),
        in_specs=[anywhere] * 2,
        out_specs=(in_vmem,) * 3,
        scratch_shapes=[
            vmem(POPS, *flat),
            vmem(STEPS, POPS, (planes + 2) * rows, lanes),
            vmem(STEPS, 2, FACE, *tile),
            vmem(STEPS, 2, FACE, *tile),
            vmem(STEPS, 2, *tile),
            vmem(STEPS, 2, *tile),
            vmem(STEPS, len(XZ), *tile),
            vmem(STEPS, len(EDGE), 1, lanes),
            vmem(STEPS, len(EDGE), 1, lanes),
            vmem(1, 1, lanes),
            vmem(nx * ny * nz, 1, lanes),
            dma((6,)),
            dma((STEPS, len(MESSAGES))),
            dma((STEPS, len(MESSAGES))),
            dma((1 + nx // 2,)),
            dma((1,)),
            dma((1,)),
            dma((1,)),
        ],
        compiler_params=pltpu.CompilerParams(collective_id=0, has_side_effects=True),
        name="lattice_steps",
    )(flow_pops.reshape((FLOWS,) + flat), heat_pops.reshape((7,) + flat))
    cells = nx * ny * nz * planes * rows * lanes
    scale = nz * lanes / (DIFFUSIVITY * (HOT_WALL - COLD_WALL)) / cells
    flow, heat, nusselt = pl.pallas_call(
        functools.partial(write_out, scale),
        out_shape=(
            jax.ShapeDtypeStruct((FLOWS,) + flat, jnp.float32),
            jax.ShapeDtypeStruct((7,) + flat, jnp.float32),
            jax.ShapeDtypeStruct((1, 1), jnp.float32),
        ),
        in_specs=[in_vmem] * 3,
        out_specs=(anywhere, anywhere, pl.BlockSpec(memory_space=pltpu.SMEM)),
        scratch_shapes=[dma((2,))],
        name="write_out",
    )(*(pltpu.with_memory_space_constraint(a, pltpu.VMEM) for a in state))
    return flow.reshape(flow_pops.shape), heat.reshape(heat_pops.shape), nusselt.reshape(())


def solution(mesh):
    shape = tuple(mesh.shape[a] for a in AXES)
    spec = P(None, *AXES)
    return jax.shard_map(
        functools.partial(per_device, shape),
        mesh=mesh,
        in_specs=(spec, spec),
        out_specs=(spec, spec, P()),
        check_vma=False,
    )
```

```python
import functools

import jax
import jax.numpy as jnp
import numpy as np
from jax import lax
from jax.experimental import pallas as pl
from jax.experimental.pallas import tpu as pltpu
from jax.sharding import PartitionSpec as P

MESH = pl.DeviceIdType.MESH
STEPS = 3
AXES = ("gx", "gy", "gz")

FLOW_SET = [
    (0, 0, 0),
    (1, 0, 0),
    (-1, 0, 0),
    (0, 1, 0),
    (0, -1, 0),
    (0, 0, 1),
    (0, 0, -1),
    (1, 1, 0),
    (-1, -1, 0),
    (1, -1, 0),
    (-1, 1, 0),
    (1, 0, 1),
    (-1, 0, -1),
    (1, 0, -1),
    (-1, 0, 1),
    (0, 1, 1),
    (0, -1, -1),
    (0, 1, -1),
    (0, -1, 1),
]
LATTICE = FLOW_SET + FLOW_SET[:7]
FLOWS = len(FLOW_SET)
POPS = len(LATTICE)
TAU_FLOW = 0.6
TAU_HEAT = 0.7
GRAVITY_LIFT = 0.01
HOT_WALL = 0.5
COLD_WALL = -0.5
DIFFUSIVITY = (TAU_HEAT - 0.5) / 4.0


def opposite(q):
    c = tuple(-v for v in LATTICE[q])
    return FLOW_SET.index(c) + (FLOWS if q >= FLOWS else 0)


def movers(axis, sign):
    return [q for q in range(POPS) if LATTICE[q][axis] == sign]


XP, XM = movers(0, 1), movers(0, -1)
YM = {1: movers(1, 1), -1: movers(1, -1)}
ZM = {1: movers(2, 1), -1: movers(2, -1)}
FACE = len(XP)
ORDER = XP + XM + [q for q in range(POPS) if LATTICE[q][0] == 0]
POS = {q: i for i, q in enumerate(ORDER)}
XY = [q for q in range(FLOWS) if LATTICE[q][0] != 0 and LATTICE[q][1] != 0]
XZ = [q for q in range(FLOWS) if LATTICE[q][0] != 0 and LATTICE[q][2] != 0]
LANE0 = 8


def messages():
    out = [("x", 1, (1, 0, 0)), ("x", -1, (-1, 0, 0))]
    out += [("xz", q, LATTICE[q]) for q in XZ]
    out += [("xy", q, LATTICE[q]) for q in XY]
    out += [("yz", (cz, cy), (0, cy, cz)) for cz in (1, -1) for cy in (1, -1)]
    out += [("z", cz, (0, 0, cz)) for cz in (1, -1)]
    out += [("y", 1, (0, 1, 0)), ("y", -1, (0, -1, 0))]
    return out


MESSAGES = messages()
EDGE = {m[:2]: i for i, m in enumerate(m for m in MESSAGES if m[0] in ("xy", "yz"))}
END_PLANES = ("x", "xy", "xz")
ALL_PLANES = ("y", "z", "yz")


def collide(f):
    s, d = {}, {}
    for q in range(1, FLOWS, 2):
        s[q] = f[q] + f[q + 1]
        d[q] = f[q] - f[q + 1]
    rho = (((s[1] + s[3]) + (s[5] + s[7])) + ((s[9] + s[11]) + (s[13] + s[15]))) + (s[17] + f[0])
    jx = (d[1] + d[7]) + (d[9] + d[11]) + d[13]
    jy = (d[3] + d[7]) + (d[15] + d[17]) - d[9]
    jz = (d[5] + d[11]) + (d[15] - d[13]) - d[17]
    g = [f[FLOWS + i] for i in range(7)]
    warmth = ((g[0] + g[1]) + (g[2] + g[3])) + ((g[4] + g[5]) + g[6])
    force = GRAVITY_LIFT * rho * warmth
    inv = 1.0 / rho
    ux = jx * inv
    uy = jy * inv
    uz = (jz + 0.5 * force) * inv

    w2 = 1.0 / 36.0
    keep = 1.0 - 1.0 / TAU_FLOW
    r = (w2 / TAU_FLOW) * rho
    sf = (w2 * (1.0 - 0.5 / TAU_FLOW)) * force
    r3 = 3.0 * r
    rx, ry, rz = r3 * ux, r3 * uy, r3 * uz
    sf3 = 3.0 * sf
    ax, ay, az = rx, ry, rz + sf3
    bx, by, bz = 1.5 * rx, 1.5 * ry, 1.5 * rz + 3.0 * sf3
    qx, qy, qz = ux * bx, uy * by, uz * bz
    usq = rx * ux + ry * uy + rz * uz
    base = r - 0.5 * usq - sf3 * uz
    cxy = ux * by + uy * bx
    cxz = ux * bz + uz * bx
    cyz = uy * bz + uz * by

    out = {0: keep * f[0] + 12.0 * base}

    def pair(q, even, odd):
        out[q] = keep * f[q] + (even + odd)
        out[q + 1] = keep * f[q + 1] + (even - odd)

    pair(1, 2.0 * (base + qx), 2.0 * ax)
    pair(3, 2.0 * (base + qy), 2.0 * ay)
    pair(5, 2.0 * (base + qz), 2.0 * az)
    exy = base + (qx + qy)
    exz = base + (qx + qz)
    eyz = base + (qy + qz)
    pair(7, exy + cxy, ax + ay)
    pair(9, exy - cxy, ax - ay)
    pair(11, exz + cxz, ax + az)
    pair(13, exz - cxz, ax - az)
    pair(15, eyz + cyz, ay + az)
    pair(17, eyz - cyz, ay - az)

    keep_heat = 1.0 - 1.0 / TAU_HEAT
    t8 = (0.125 / TAU_HEAT) * warmth
    t2 = 4.0 * t8
    out[FLOWS] = keep_heat * g[0] + 2.0 * t8
    for i, u in ((1, ux), (3, uy), (5, uz)):
        odd = t2 * u
        out[FLOWS + i] = keep_heat * g[i] + (t8 + odd)
        out[FLOWS + i + 1] = keep_heat * g[i + 1] + (t8 - odd)
    return out


def flux(f):
    total = lambda values: functools.reduce(lambda a, b: a + b, values)
    rho = total([f[q] for q in range(FLOWS)])
    jz = total([f[q] for q in range(FLOWS) if LATTICE[q][2] == 1]) - total(
        [f[q] for q in range(FLOWS) if LATTICE[q][2] == -1]
    )
    warmth = total([f[q] for q in range(FLOWS, POPS)])
    force = GRAVITY_LIFT * rho * warmth
    return (jz + 0.5 * force) / rho * warmth


def kernel(
    shape,
    sizes,
    flow_in,
    heat_in,
    flow_out,
    heat_out,
    total,
    held,
    post,
    ysend,
    yrecv,
    zsend,
    zrecv,
    zdiag,
    edge_send,
    edge_recv,
    part,
    parts,
    in_sem,
    send_sem,
    recv_sem,
    part_send,
    part_recv,
    total_send,
    total_recv,
):
    nx, ny, nz = shape
    planes, rows, lanes = sizes
    me = tuple(lax.axis_index(a) for a in AXES)
    count = nx * ny * nz
    group = ny * nz
    my_index = me[0] * group + me[1] * nz + me[2]
    is_root = lax.rem(me[0], nx // 2) < nx // 4

    def at(off):
        return tuple(m if d == 0 else lax.rem(m + (d % n), n) for m, d, n in zip(me, off, shape))

    offsets = [off for off in np.ndindex(3, 3, 3) if off != (1, 1, 1)]
    offsets = [tuple(d - 1 for d in off) for off in offsets if 1 in off]
    barrier = pltpu.get_barrier_semaphore()
    for off in offsets:
        pl.semaphore_signal(barrier, inc=1, device_id=at(off), device_id_type=MESH)

    inner, ends = range(1, planes - 1), (0, planes - 1)
    blocks = [(0, 1), (planes - 1, 1), (1, planes - 2)]
    loads = []
    for i, (x, n) in enumerate(blocks):
        some = pl.ds(x * rows, n * rows)
        for j, (ref, low, n) in enumerate(((flow_in, 0, FLOWS), (heat_in, FLOWS, 7))):
            loads.append(
                pltpu.make_async_copy(ref.at[:, some], held.at[pl.ds(low, n), some], in_sem.at[2 * i + j])
            )
    for c in loads:
        c.start()

    @pl.when(is_root)
    def _():
        for d in range(1, nx):
            pl.semaphore_signal(barrier, inc=1, device_id=at((d, 0, 0)), device_id_type=MESH)

    lane = lax.broadcasted_iota(jnp.int32, (rows, lanes), 1)
    row = lax.broadcasted_iota(jnp.int32, (rows, lanes), 0)
    is_bottom = me[2] == 0
    is_top = me[2] == nz - 1
    end_lane = {1: lane == 0, -1: lane == lanes - 1}
    wall = {1: jnp.logical_and(end_lane[1], is_bottom), -1: jnp.logical_and(end_lane[-1], is_top)}
    end_row = {1: row == 0, -1: row == rows - 1}
    far_row = {1: rows - 1, -1: 0}
    side = {1: 0, -1: 1}

    def turn(v, c, axis):
        n = rows if axis == 0 else lanes
        return pltpu.roll(v, 1 if c == 1 else n - 1, axis)

    def plane(x):
        return pl.ds((x + 1) * rows, rows)

    def keep(s, x, out, packed):
        if x in ends:
            cx = 1 if x else -1
            for q in XY:
                if LATTICE[q][0] == cx:
                    far = far_row[LATTICE[q][1]]
                    edge_send[s, EDGE["xy", q]] = out[q][far : far + 1, :]
        for q in range(POPS):
            post[s, POS[q], plane(x), :] = out[q]
        for cz in (1, -1):
            for j, q in enumerate(ZM[cz]):
                k = LANE0 + j * planes + x
                packed[cz] = jnp.where(lane == k, pltpu.roll(out[q], k + (1 if cz == 1 else 0), 1), packed[cz])

    def crew(end, dz):
        return (0 if end else 3) + dz + 1

    def copy(s, m):
        kind, slot, off = MESSAGES[m]
        if kind == "x":
            some = pl.ds(0 if slot == 1 else FACE, FACE)
            src, dst = (planes - 1, -1) if slot == 1 else (0, planes)
            src, dst = post.at[s, some, plane(src)], post.at[s, some, plane(dst)]
        elif kind == "y":
            src, dst = ysend.at[s, side[slot]], yrecv.at[s, side[slot]]
        elif kind == "z":
            src, dst = zsend.at[s, side[slot]], zrecv.at[s, side[slot]]
        elif kind == "xz":
            src = post.at[s, POS[slot], plane(planes - 1 if off[0] == 1 else 0)]
            dst = zdiag.at[s, XZ.index(slot)]
        else:
            src, dst = edge_send.at[s, EDGE[kind, slot]], edge_recv.at[s, EDGE[kind, slot]]
        return pltpu.make_async_remote_copy(
            src_ref=src,
            dst_ref=dst,
            send_sem=send_sem.at[s, crew(kind in END_PLANES, off[2])],
            recv_sem=recv_sem.at[s, crew(kind in END_PLANES, off[2])],
            device_id=at(off),
            device_id_type=MESH,
        )

    def of_kind(kinds, dz):
        return [m for m, (kind, _, off) in enumerate(MESSAGES) if kind in kinds and off[2] == dz]

    def each(act, up, down):
        for dz, when in ((1, up), (-1, down)):

            @pl.when(when)
            def _():
                act(dz)

        act(0)

    def start(s, kinds):
        def act(dz):
            for m in of_kind(kinds, dz):
                copy(s, m).start()

        each(act, jnp.logical_not(is_top), jnp.logical_not(is_bottom))

    def bytes_of(s, kinds, dz):
        size = {"x": FACE * rows, "y": FACE * planes, "z": rows, "xz": rows, "xy": 1, "yz": 1}
        some = parts.at[pl.ds(0, sum(size[MESSAGES[m][0]] for m in of_kind(kinds, dz)))]
        return pltpu.make_async_remote_copy(
            src_ref=some,
            dst_ref=some,
            send_sem=send_sem.at[s, crew(kinds == END_PLANES, dz)],
            recv_sem=recv_sem.at[s, crew(kinds == END_PLANES, dz)],
            device_id=at((1, 0, 0)),
            device_id_type=MESH,
        )

    def receive(s, kinds):
        each(lambda dz: bytes_of(s, kinds, dz).wait_recv(), jnp.logical_not(is_bottom), jnp.logical_not(is_top))

    def drain(s, kinds):
        each(lambda dz: bytes_of(s, kinds, dz).wait_send(), jnp.logical_not(is_top), jnp.logical_not(is_bottom))

    def pack(s, packed):
        for cy in (1, -1):
            first = rows + far_row[cy]
            for j, q in enumerate(YM[cy]):
                ysend[s, side[cy], j] = post[s, POS[q], pl.ds(first, planes, stride=rows), :]
        for cz in (1, -1):
            zsend[s, side[cz]] = packed[cz]
            for cy in (1, -1):
                far = far_row[cy]
                edge_send[s, EDGE["yz", (cz, cy)]] = packed[cz][far : far + 1, :]

    def z_faces(s):
        tiles = {}
        for cz in (1, -1):
            own = zrecv[s, side[cz]]
            tiles[cz, 0] = own
            for cy in (1, -1):
                other = jnp.broadcast_to(edge_recv[s, EDGE["yz", (cz, cy)]], (rows, lanes))
                tiles[cz, cy] = jnp.where(end_row[cy], other, turn(own, cy, 0))
        return tiles

    def stream(s, x, tiles):
        f = {}
        for q in range(POPS):
            cx, cy, cz = LATTICE[q]
            v = post[s, POS[q], plane(x - cx), :]
            inside = 0 <= x - cx < planes
            if cy:
                if inside:
                    edge = yrecv[s, side[cy], YM[cy].index(q), pl.ds(x - cx, 1), :]
                else:
                    edge = edge_recv[s, EDGE["xy", q]]
                v = jnp.where(end_row[cy], jnp.broadcast_to(edge, (rows, lanes)), turn(v, cy, 0))
            if cz:
                if inside:
                    k = LANE0 + ZM[cz].index(q) * planes + x - cx
                    edge = pltpu.roll(tiles[cz, cy], (lanes if cz == 1 else lanes - 1) - k, 1)
                else:
                    edge = turn(zdiag[s, XZ.index(q)], cz, 1)
                back = post[s, POS[opposite(q)], plane(x), :]
                if q >= FLOWS:
                    back = 0.25 * (HOT_WALL if cz == 1 else COLD_WALL) - back
                v = jnp.where(wall[cz], back, jnp.where(end_lane[cz], edge, turn(v, cz, 1)))
            f[q] = v
        return f

    blank = jnp.zeros((rows, lanes), jnp.float32)

    def first(x, packed):
        keep(0, x, collide({q: held[q, pl.ds(x * rows, rows), :] for q in range(POPS)}), packed)

    packed = {1: blank, -1: blank}
    for c in loads[:4]:
        c.wait()
    for x in ends:
        first(x, packed)
    pl.semaphore_wait(barrier, len(offsets) + nx // 2 - is_root.astype(jnp.int32))
    start(0, END_PLANES)
    for c in loads[4:]:
        c.wait()
    for x in inner:
        first(x, packed)
    pack(0, packed)
    start(0, ALL_PLANES)

    for s in range(1, STEPS):
        packed = {1: blank, -1: blank}
        receive(s - 1, ALL_PLANES)
        tiles = z_faces(s - 1)
        for x in inner:
            keep(s, x, collide(stream(s - 1, x, tiles)), packed)
        receive(s - 1, END_PLANES)
        for x in ends:
            keep(s, x, collide(stream(s - 1, x, tiles)), packed)
        start(s, END_PLANES)
        pack(s, packed)
        start(s, ALL_PLANES)

    def last(x, tiles):
        f = stream(STEPS - 1, x, tiles)
        for q in range(FLOWS):
            flow_out[q, pl.ds(x * rows, rows), :] = f[q]
        for q in range(FLOWS, POPS):
            heat_out[q - FLOWS, pl.ds(x * rows, rows), :] = f[q]
        return flux(f)

    receive(STEPS - 1, ALL_PLANES)
    tiles = z_faces(STEPS - 1)
    acc = blank
    for x in inner:
        acc = acc + last(x, tiles)
    receive(STEPS - 1, END_PLANES)
    for x in ends:
        acc = acc + last(x, tiles)

    mine = jnp.sum(acc, axis=0, keepdims=True)
    part[0] = mine
    parts[my_index] = mine
    seat = lax.rem(my_index, group)
    half = nx // 2
    lines = [x for x in range(nx) if x % half < nx // 4]

    def to_root(x, d):
        return pltpu.make_async_remote_copy(
            src_ref=part.at[0],
            dst_ref=parts.at[my_index],
            send_sem=part_send.at[0],
            recv_sem=part_recv.at[0],
            device_id=x * group + lax.rem(seat + d, group),
            device_id_type=pl.DeviceIdType.LOGICAL,
        )

    for x in lines:

        @pl.when(me[0] != x)
        def _():
            to_root(x, 0).start()

        for d in range(1, group):
            to_root(x, d).start()

    served = [half - 1 - lax.rem(me[0], half) + half * lax.div(me[0], half)]

    def to_served(i):
        return pltpu.make_async_remote_copy(
            src_ref=total.at[0],
            dst_ref=total.at[0],
            send_sem=total_send.at[i],
            recv_sem=total_recv.at[0],
            device_id=(served[i], me[1], me[2]),
            device_id_type=MESH,
        )

    def whole(n, k):
        some = parts.at[pl.ds(0, n)]
        return pltpu.make_async_remote_copy(
            src_ref=some,
            dst_ref=some,
            send_sem=part_send.at[k],
            recv_sem=part_recv.at[0],
            device_id=0,
            device_id_type=pl.DeviceIdType.LOGICAL,
        )

    for s in range(STEPS):
        drain(s, END_PLANES)
        drain(s, ALL_PLANES)

    @pl.when(is_root)
    def _():
        whole(len(lines) * group - 1, 0).wait_send()

    @pl.when(jnp.logical_not(is_root))
    def _():
        whole(len(lines) * group, 0).wait_send()

    @pl.when(is_root)
    def _():
        whole(count - 1, 0).wait_recv()
        sums = [parts[i] for i in range(8)]
        for i in range(8, count):
            sums[i % 8] = sums[i % 8] + parts[i]
        total[0] = ((sums[0] + sums[1]) + (sums[2] + sums[3])) + ((sums[4] + sums[5]) + (sums[6] + sums[7]))
        for i in range(1):
            to_served(i).start()

    @pl.when(jnp.logical_not(is_root))
    def _():
        to_served(0).wait_recv()

    @pl.when(is_root)
    def _():
        for i in range(1):
            to_served(i).wait_send()


def write_out(scale, flow, heat, total, flow_out, heat_out, nusselt, value, sem):
    copies = [
        pltpu.make_async_copy(flow, flow_out, sem.at[0]),
        pltpu.make_async_copy(heat, heat_out, sem.at[1]),
    ]
    for c in copies:
        c.start()
    value[...] = 1.0 + scale * jnp.sum(total[0], axis=1, keepdims=True)
    copies.append(pltpu.make_async_copy(value, nusselt, sem.at[2]))
    copies[2].start()
    for c in copies:
        c.wait()


def per_device(shape, flow_pops, heat_pops):
    nx, ny, nz = shape
    _, planes, rows, lanes = flow_pops.shape
    flat = (planes * rows, lanes)
    dma = pltpu.SemaphoreType.DMA
    tile = (rows, lanes)
    vmem = lambda *dims: pltpu.VMEM(dims, jnp.float32)
    anywhere = pl.BlockSpec(memory_space=pl.ANY)
    in_vmem = pl.BlockSpec(memory_space=pltpu.VMEM)
    state = pl.pallas_call(
        functools.partial(kernel, shape, (planes, rows, lanes)),
        out_shape=(
            vmem(FLOWS, *flat),
            vmem(7, *flat),
            vmem(1, 1, lanes),
        ),
        in_specs=[anywhere] * 2,
        out_specs=(in_vmem,) * 3,
        scratch_shapes=[
            vmem(POPS, *flat),
            vmem(STEPS, POPS, (planes + 2) * rows, lanes),
            vmem(STEPS, 2, FACE, *tile),
            vmem(STEPS, 2, FACE, *tile),
            vmem(STEPS, 2, *tile),
            vmem(STEPS, 2, *tile),
            vmem(STEPS, len(XZ), *tile),
            vmem(STEPS, len(EDGE), 1, lanes),
            vmem(STEPS, len(EDGE), 1, lanes),
            vmem(1, 1, lanes),
            vmem(max(nx * ny * nz, 128), 1, lanes),
            dma((6,)),
            dma((STEPS, 6)),
            dma((STEPS, 6)),
            dma((1,)),
            dma((1,)),
            dma((1,)),
            dma((1,)),
        ],
        compiler_params=pltpu.CompilerParams(collective_id=0, has_side_effects=True),
        name="lattice_steps",
    )(flow_pops.reshape((FLOWS,) + flat), heat_pops.reshape((7,) + flat))
    cells = nx * ny * nz * planes * rows * lanes
    scale = nz * lanes / (DIFFUSIVITY * (HOT_WALL - COLD_WALL)) / cells
    flow, heat, nusselt = pl.pallas_call(
        functools.partial(write_out, scale),
        out_shape=(
            jax.ShapeDtypeStruct((FLOWS,) + flat, jnp.float32),
            jax.ShapeDtypeStruct((7,) + flat, jnp.float32),
            jax.ShapeDtypeStruct((1, 1), jnp.float32),
        ),
        in_specs=[in_vmem] * 3,
        out_specs=(anywhere,) * 3,
        scratch_shapes=[vmem(1, 1), dma((3,))],
        name="write_out",
    )(*(pltpu.with_memory_space_constraint(a, pltpu.VMEM) for a in state))
    return flow.reshape(flow_pops.shape), heat.reshape(heat_pops.shape), nusselt.reshape(())


def solution(mesh):
    shape = tuple(mesh.shape[a] for a in AXES)
    spec = P(None, *AXES)
    return jax.shard_map(
        functools.partial(per_device, shape),
        mesh=mesh,
        in_specs=(spec, spec),
        out_specs=(spec, spec, P()),
        check_vma=False,
    )
```

```python
import functools

import jax
import jax.numpy as jnp
import numpy as np
from jax import lax
from jax.experimental import pallas as pl
from jax.experimental.pallas import tpu as pltpu
from jax.sharding import PartitionSpec as P

MESH = pl.DeviceIdType.MESH
STEPS = 3
AXES = ("gx", "gy", "gz")

FLOW_SET = [
    (0, 0, 0),
    (1, 0, 0),
    (-1, 0, 0),
    (0, 1, 0),
    (0, -1, 0),
    (0, 0, 1),
    (0, 0, -1),
    (1, 1, 0),
    (-1, -1, 0),
    (1, -1, 0),
    (-1, 1, 0),
    (1, 0, 1),
    (-1, 0, -1),
    (1, 0, -1),
    (-1, 0, 1),
    (0, 1, 1),
    (0, -1, -1),
    (0, 1, -1),
    (0, -1, 1),
]
LATTICE = FLOW_SET + FLOW_SET[:7]
FLOWS = len(FLOW_SET)
POPS = len(LATTICE)
TAU_FLOW = 0.6
TAU_HEAT = 0.7
GRAVITY_LIFT = 0.01
HOT_WALL = 0.5
COLD_WALL = -0.5
DIFFUSIVITY = (TAU_HEAT - 0.5) / 4.0


def opposite(q):
    c = tuple(-v for v in LATTICE[q])
    return FLOW_SET.index(c) + (FLOWS if q >= FLOWS else 0)


def movers(axis, sign):
    return [q for q in range(POPS) if LATTICE[q][axis] == sign]


XP, XM = movers(0, 1), movers(0, -1)
YM = {1: movers(1, 1), -1: movers(1, -1)}
ZM = {1: movers(2, 1), -1: movers(2, -1)}
FACE = len(XP)
ORDER = XP + XM + [q for q in range(POPS) if LATTICE[q][0] == 0]
POS = {q: i for i, q in enumerate(ORDER)}
XY = [q for q in range(FLOWS) if LATTICE[q][0] != 0 and LATTICE[q][1] != 0]
XZ = [q for q in range(FLOWS) if LATTICE[q][0] != 0 and LATTICE[q][2] != 0]
LANE0 = 8


def messages():
    out = [("x", 1, (1, 0, 0)), ("x", -1, (-1, 0, 0))]
    out += [("xz", q, LATTICE[q]) for q in XZ]
    out += [("xy", q, LATTICE[q]) for q in XY]
    out += [("yz", (cz, cy), (0, cy, cz)) for cz in (1, -1) for cy in (1, -1)]
    out += [("z", cz, (0, 0, cz)) for cz in (1, -1)]
    out += [("y", 1, (0, 1, 0)), ("y", -1, (0, -1, 0))]
    return out


MESSAGES = messages()
EDGE = {m[:2]: i for i, m in enumerate(m for m in MESSAGES if m[0] in ("xy", "yz"))}
END_PLANES = ("x", "xy", "xz")
ALL_PLANES = ("y", "z", "yz")


def collide(f):
    s, d = {}, {}
    for q in range(1, FLOWS, 2):
        s[q] = f[q] + f[q + 1]
        d[q] = f[q] - f[q + 1]
    rho = (((s[1] + s[3]) + (s[5] + s[7])) + ((s[9] + s[11]) + (s[13] + s[15]))) + (s[17] + f[0])
    jx = (d[1] + d[7]) + (d[9] + d[11]) + d[13]
    jy = (d[3] + d[7]) + (d[15] + d[17]) - d[9]
    jz = (d[5] + d[11]) + (d[15] - d[13]) - d[17]
    g = [f[FLOWS + i] for i in range(7)]
    warmth = ((g[0] + g[1]) + (g[2] + g[3])) + ((g[4] + g[5]) + g[6])
    force = GRAVITY_LIFT * rho * warmth
    inv = 1.0 / rho
    ux = jx * inv
    uy = jy * inv
    uz = (jz + 0.5 * force) * inv

    w2 = 1.0 / 36.0
    keep = 1.0 - 1.0 / TAU_FLOW
    r = (w2 / TAU_FLOW) * rho
    sf = (w2 * (1.0 - 0.5 / TAU_FLOW)) * force
    r3 = 3.0 * r
    rx, ry, rz = r3 * ux, r3 * uy, r3 * uz
    sf3 = 3.0 * sf
    ax, ay, az = rx, ry, rz + sf3
    bx, by, bz = 1.5 * rx, 1.5 * ry, 1.5 * rz + 3.0 * sf3
    qx, qy, qz = ux * bx, uy * by, uz * bz
    usq = rx * ux + ry * uy + rz * uz
    base = r - 0.5 * usq - sf3 * uz
    cxy = ux * by + uy * bx
    cxz = ux * bz + uz * bx
    cyz = uy * bz + uz * by

    out = {0: keep * f[0] + 12.0 * base}

    def pair(q, even, odd):
        out[q] = keep * f[q] + (even + odd)
        out[q + 1] = keep * f[q + 1] + (even - odd)

    pair(1, 2.0 * (base + qx), 2.0 * ax)
    pair(3, 2.0 * (base + qy), 2.0 * ay)
    pair(5, 2.0 * (base + qz), 2.0 * az)
    exy = base + (qx + qy)
    exz = base + (qx + qz)
    eyz = base + (qy + qz)
    pair(7, exy + cxy, ax + ay)
    pair(9, exy - cxy, ax - ay)
    pair(11, exz + cxz, ax + az)
    pair(13, exz - cxz, ax - az)
    pair(15, eyz + cyz, ay + az)
    pair(17, eyz - cyz, ay - az)

    keep_heat = 1.0 - 1.0 / TAU_HEAT
    t8 = (0.125 / TAU_HEAT) * warmth
    t2 = 4.0 * t8
    out[FLOWS] = keep_heat * g[0] + 2.0 * t8
    for i, u in ((1, ux), (3, uy), (5, uz)):
        odd = t2 * u
        out[FLOWS + i] = keep_heat * g[i] + (t8 + odd)
        out[FLOWS + i + 1] = keep_heat * g[i + 1] + (t8 - odd)
    return out


def flux(f):
    total = lambda values: functools.reduce(lambda a, b: a + b, values)
    rho = total([f[q] for q in range(FLOWS)])
    jz = total([f[q] for q in range(FLOWS) if LATTICE[q][2] == 1]) - total(
        [f[q] for q in range(FLOWS) if LATTICE[q][2] == -1]
    )
    warmth = total([f[q] for q in range(FLOWS, POPS)])
    force = GRAVITY_LIFT * rho * warmth
    return (jz + 0.5 * force) / rho * warmth


def kernel(
    shape,
    sizes,
    flow_in,
    heat_in,
    flow_out,
    heat_out,
    total,
    held,
    post,
    ysend,
    yrecv,
    zsend,
    zrecv,
    zdiag,
    edge_send,
    edge_recv,
    part,
    parts,
    in_sem,
    send_sem,
    recv_sem,
    part_send,
    part_recv,
    total_send,
    total_recv,
):
    nx, ny, nz = shape
    planes, rows, lanes = sizes
    me = tuple(lax.axis_index(a) for a in AXES)
    count = nx * ny * nz
    group = ny * nz
    lines = nx - nx // 4
    my_index = me[0] * group + me[1] * nz + me[2]
    is_root = me[0] < lines

    def at(off):
        return tuple(m if d == 0 else lax.rem(m + (d % n), n) for m, d, n in zip(me, off, shape))

    offsets = [off for off in np.ndindex(3, 3, 3) if off != (1, 1, 1)]
    offsets = [tuple(d - 1 for d in off) for off in offsets if 1 in off]
    offsets.sort(key=lambda off: -2 * abs(off[0]) - abs(off[2]))
    barrier = pltpu.get_barrier_semaphore()
    for off in offsets:
        pl.semaphore_signal(barrier, inc=1, device_id=at(off), device_id_type=MESH)

    inner, ends = range(1, planes - 1), (0, planes - 1)
    blocks = [(0, 1), (planes - 1, 1), (1, planes - 2)]
    loads = []
    for i, (x, n) in enumerate(blocks):
        some = pl.ds(x * rows, n * rows)
        for j, (ref, low, n) in enumerate(((flow_in, 0, FLOWS), (heat_in, FLOWS, 7))):
            loads.append(
                pltpu.make_async_copy(ref.at[:, some], held.at[pl.ds(low, n), some], in_sem.at[2 * i + j])
            )
    for c in loads:
        c.start()

    @pl.when(is_root)
    def _():
        for d in range(1, nx):
            pl.semaphore_signal(barrier, inc=1, device_id=at((d, 0, 0)), device_id_type=MESH)

    lane = lax.broadcasted_iota(jnp.int32, (rows, lanes), 1)
    row = lax.broadcasted_iota(jnp.int32, (rows, lanes), 0)
    is_bottom = me[2] == 0
    is_top = me[2] == nz - 1
    end_lane = {1: lane == 0, -1: lane == lanes - 1}
    wall = {1: jnp.logical_and(end_lane[1], is_bottom), -1: jnp.logical_and(end_lane[-1], is_top)}
    end_row = {1: row == 0, -1: row == rows - 1}
    far_row = {1: rows - 1, -1: 0}
    side = {1: 0, -1: 1}

    def turn(v, c, axis):
        n = rows if axis == 0 else lanes
        return pltpu.roll(v, 1 if c == 1 else n - 1, axis)

    def plane(x):
        return pl.ds((x + 1) * rows, rows)

    def keep(s, x, out, packed):
        if x in ends:
            cx = 1 if x else -1
            for q in XY:
                if LATTICE[q][0] == cx:
                    far = far_row[LATTICE[q][1]]
                    edge_send[s, EDGE["xy", q]] = out[q][far : far + 1, :]
        for q in range(POPS):
            post[s, POS[q], plane(x), :] = out[q]
        for cz in (1, -1):
            for j, q in enumerate(ZM[cz]):
                k = LANE0 + j * planes + x
                packed[cz] = jnp.where(lane == k, pltpu.roll(out[q], k + (1 if cz == 1 else 0), 1), packed[cz])

    def crew(end, dz):
        return (0 if end else 3) + dz + 1

    def copy(s, m):
        kind, slot, off = MESSAGES[m]
        if kind == "x":
            some = pl.ds(0 if slot == 1 else FACE, FACE)
            src, dst = (planes - 1, -1) if slot == 1 else (0, planes)
            src, dst = post.at[s, some, plane(src)], post.at[s, some, plane(dst)]
        elif kind == "y":
            src, dst = ysend.at[s, side[slot]], yrecv.at[s, side[slot]]
        elif kind == "z":
            src, dst = zsend.at[s, side[slot]], zrecv.at[s, side[slot]]
        elif kind == "xz":
            src = post.at[s, POS[slot], plane(planes - 1 if off[0] == 1 else 0)]
            dst = zdiag.at[s, XZ.index(slot)]
        else:
            src, dst = edge_send.at[s, EDGE[kind, slot]], edge_recv.at[s, EDGE[kind, slot]]
        return pltpu.make_async_remote_copy(
            src_ref=src,
            dst_ref=dst,
            send_sem=send_sem.at[s, crew(kind in END_PLANES, off[2])],
            recv_sem=recv_sem.at[s, crew(kind in END_PLANES, off[2])],
            device_id=at(off),
            device_id_type=MESH,
        )

    def of_kind(kinds, dz):
        return [m for m, (kind, _, off) in enumerate(MESSAGES) if kind in kinds and off[2] == dz]

    def each(act, up, down):
        for dz, when in ((1, up), (-1, down)):

            @pl.when(when)
            def _():
                act(dz)

        act(0)

    def start(s, kinds):
        def act(dz):
            for m in of_kind(kinds, dz):
                copy(s, m).start()

        each(act, jnp.logical_not(is_top), jnp.logical_not(is_bottom))

    def bytes_of(s, kinds, dz):
        size = {"x": FACE * rows, "y": FACE * planes, "z": rows, "xz": rows, "xy": 1, "yz": 1}
        some = parts.at[pl.ds(0, sum(size[MESSAGES[m][0]] for m in of_kind(kinds, dz)))]
        return pltpu.make_async_remote_copy(
            src_ref=some,
            dst_ref=some,
            send_sem=send_sem.at[s, crew(kinds == END_PLANES, dz)],
            recv_sem=recv_sem.at[s, crew(kinds == END_PLANES, dz)],
            device_id=at((1, 0, 0)),
            device_id_type=MESH,
        )

    def receive(s, kinds):
        each(lambda dz: bytes_of(s, kinds, dz).wait_recv(), jnp.logical_not(is_bottom), jnp.logical_not(is_top))

    def drain(s, kinds):
        each(lambda dz: bytes_of(s, kinds, dz).wait_send(), jnp.logical_not(is_top), jnp.logical_not(is_bottom))

    def pack(s, packed):
        for cy in (1, -1):
            first = rows + far_row[cy]
            for j, q in enumerate(YM[cy]):
                ysend[s, side[cy], j] = post[s, POS[q], pl.ds(first, planes, stride=rows), :]
        for cz in (1, -1):
            zsend[s, side[cz]] = packed[cz]
            for cy in (1, -1):
                far = far_row[cy]
                edge_send[s, EDGE["yz", (cz, cy)]] = packed[cz][far : far + 1, :]

    def z_faces(s):
        tiles = {}
        for cz in (1, -1):
            own = zrecv[s, side[cz]]
            tiles[cz, 0] = own
            for cy in (1, -1):
                other = jnp.broadcast_to(edge_recv[s, EDGE["yz", (cz, cy)]], (rows, lanes))
                tiles[cz, cy] = jnp.where(end_row[cy], other, turn(own, cy, 0))
        return tiles

    def stream(s, x, tiles):
        f = {}
        for q in range(POPS):
            cx, cy, cz = LATTICE[q]
            v = post[s, POS[q], plane(x - cx), :]
            inside = 0 <= x - cx < planes
            if cy:
                if inside:
                    edge = yrecv[s, side[cy], YM[cy].index(q), pl.ds(x - cx, 1), :]
                else:
                    edge = edge_recv[s, EDGE["xy", q]]
                v = jnp.where(end_row[cy], jnp.broadcast_to(edge, (rows, lanes)), turn(v, cy, 0))
            if cz:
                if inside:
                    k = LANE0 + ZM[cz].index(q) * planes + x - cx
                    edge = pltpu.roll(tiles[cz, cy], (lanes if cz == 1 else lanes - 1) - k, 1)
                else:
                    edge = turn(zdiag[s, XZ.index(q)], cz, 1)
                back = post[s, POS[opposite(q)], plane(x), :]
                if q >= FLOWS:
                    back = 0.25 * (HOT_WALL if cz == 1 else COLD_WALL) - back
                v = jnp.where(wall[cz], back, jnp.where(end_lane[cz], edge, turn(v, cz, 1)))
            f[q] = v
        return f

    blank = jnp.zeros((rows, lanes), jnp.float32)

    def first(x, packed):
        keep(0, x, collide({q: held[q, pl.ds(x * rows, rows), :] for q in range(POPS)}), packed)

    packed = {1: blank, -1: blank}
    for c in loads[:4]:
        c.wait()
    for x in ends:
        first(x, packed)
    pl.semaphore_wait(barrier, len(offsets) + lines - is_root.astype(jnp.int32))
    start(0, END_PLANES)
    for c in loads[4:]:
        c.wait()
    for x in inner:
        first(x, packed)
    pack(0, packed)
    start(0, ALL_PLANES)

    for s in range(1, STEPS):
        packed = {1: blank, -1: blank}
        receive(s - 1, ALL_PLANES)
        tiles = z_faces(s - 1)
        for x in inner:
            keep(s, x, collide(stream(s - 1, x, tiles)), packed)
        receive(s - 1, END_PLANES)
        for x in ends:
            keep(s, x, collide(stream(s - 1, x, tiles)), packed)
        start(s, END_PLANES)
        pack(s, packed)
        start(s, ALL_PLANES)

    def last(x, tiles):
        f = stream(STEPS - 1, x, tiles)
        for q in range(FLOWS):
            flow_out[q, pl.ds(x * rows, rows), :] = f[q]
        for q in range(FLOWS, POPS):
            heat_out[q - FLOWS, pl.ds(x * rows, rows), :] = f[q]
        return flux(f)

    receive(STEPS - 1, ALL_PLANES)
    tiles = z_faces(STEPS - 1)
    acc = blank
    for x in inner:
        acc = acc + last(x, tiles)
    receive(STEPS - 1, END_PLANES)
    for x in ends:
        acc = acc + last(x, tiles)

    mine = jnp.sum(acc, axis=0, keepdims=True)
    part[0] = mine
    parts[my_index] = mine
    seat = lax.rem(my_index, group)

    def to_root(x, d):
        return pltpu.make_async_remote_copy(
            src_ref=part.at[0],
            dst_ref=parts.at[my_index],
            send_sem=part_send.at[0],
            recv_sem=part_recv.at[0],
            device_id=x * group + lax.rem(seat + d, group),
            device_id_type=pl.DeviceIdType.LOGICAL,
        )

    for x in range(lines):

        @pl.when(me[0] != x)
        def _():
            to_root(x, 0).start()

        for d in range(1, group):
            to_root(x, d).start()

    serves = jnp.logical_and(me[0] >= nx // 2, is_root)
    served = [nx + nx // 2 - 1 - me[0]]

    def to_served(i):
        return pltpu.make_async_remote_copy(
            src_ref=total.at[0],
            dst_ref=total.at[0],
            send_sem=total_send.at[i],
            recv_sem=total_recv.at[0],
            device_id=(served[i], me[1], me[2]),
            device_id_type=MESH,
        )

    def whole(n, k):
        some = parts.at[pl.ds(0, n)]
        return pltpu.make_async_remote_copy(
            src_ref=some,
            dst_ref=some,
            send_sem=part_send.at[k],
            recv_sem=part_recv.at[0],
            device_id=0,
            device_id_type=pl.DeviceIdType.LOGICAL,
        )

    for s in range(STEPS):
        drain(s, END_PLANES)
        drain(s, ALL_PLANES)

    @pl.when(is_root)
    def _():
        whole(lines * group - 1, 0).wait_send()

    @pl.when(jnp.logical_not(is_root))
    def _():
        whole(lines * group, 0).wait_send()

    @pl.when(is_root)
    def _():
        whole(count - 1, 0).wait_recv()
        sums = [parts[i] for i in range(8)]
        for i in range(8, count):
            sums[i % 8] = sums[i % 8] + parts[i]
        total[0] = ((sums[0] + sums[1]) + (sums[2] + sums[3])) + ((sums[4] + sums[5]) + (sums[6] + sums[7]))

        @pl.when(serves)
        def _():
            to_served(0).start()

    @pl.when(jnp.logical_not(is_root))
    def _():
        to_served(0).wait_recv()

    @pl.when(serves)
    def _():
        to_served(0).wait_send()


def write_out(scale, flow, heat, total, flow_out, heat_out, nusselt, value, sem):
    copies = [
        pltpu.make_async_copy(flow, flow_out, sem.at[0]),
        pltpu.make_async_copy(heat, heat_out, sem.at[1]),
    ]
    for c in copies:
        c.start()
    value[...] = 1.0 + scale * jnp.sum(total[0], axis=1, keepdims=True)
    copies.append(pltpu.make_async_copy(value, nusselt, sem.at[2]))
    copies[2].start()
    for c in copies:
        c.wait()


def per_device(shape, flow_pops, heat_pops):
    nx, ny, nz = shape
    _, planes, rows, lanes = flow_pops.shape
    flat = (planes * rows, lanes)
    dma = pltpu.SemaphoreType.DMA
    tile = (rows, lanes)
    vmem = lambda *dims: pltpu.VMEM(dims, jnp.float32)
    anywhere = pl.BlockSpec(memory_space=pl.ANY)
    in_vmem = pl.BlockSpec(memory_space=pltpu.VMEM)
    state = pl.pallas_call(
        functools.partial(kernel, shape, (planes, rows, lanes)),
        out_shape=(
            vmem(FLOWS, *flat),
            vmem(7, *flat),
            vmem(1, 1, lanes),
        ),
        in_specs=[anywhere] * 2,
        out_specs=(in_vmem,) * 3,
        scratch_shapes=[
            vmem(POPS, *flat),
            vmem(STEPS, POPS, (planes + 2) * rows, lanes),
            vmem(STEPS, 2, FACE, *tile),
            vmem(STEPS, 2, FACE, *tile),
            vmem(STEPS, 2, *tile),
            vmem(STEPS, 2, *tile),
            vmem(STEPS, len(XZ), *tile),
            vmem(STEPS, len(EDGE), 1, lanes),
            vmem(STEPS, len(EDGE), 1, lanes),
            vmem(1, 1, lanes),
            vmem(max(nx * ny * nz, 128), 1, lanes),
            dma((6,)),
            dma((STEPS, 6)),
            dma((STEPS, 6)),
            dma((1,)),
            dma((1,)),
            dma((1,)),
            dma((1,)),
        ],
        compiler_params=pltpu.CompilerParams(collective_id=0, has_side_effects=True),
        name="lattice_steps",
    )(flow_pops.reshape((FLOWS,) + flat), heat_pops.reshape((7,) + flat))
    cells = nx * ny * nz * planes * rows * lanes
    scale = nz * lanes / (DIFFUSIVITY * (HOT_WALL - COLD_WALL)) / cells
    flow, heat, nusselt = pl.pallas_call(
        functools.partial(write_out, scale),
        out_shape=(
            jax.ShapeDtypeStruct((FLOWS,) + flat, jnp.float32),
            jax.ShapeDtypeStruct((7,) + flat, jnp.float32),
            jax.ShapeDtypeStruct((1, 1), jnp.float32),
        ),
        in_specs=[in_vmem] * 3,
        out_specs=(anywhere,) * 3,
        scratch_shapes=[vmem(1, 1), dma((3,))],
        name="write_out",
    )(*(pltpu.with_memory_space_constraint(a, pltpu.VMEM) for a in state))
    return flow.reshape(flow_pops.shape), heat.reshape(heat_pops.shape), nusselt.reshape(())


def solution(mesh):
    shape = tuple(mesh.shape[a] for a in AXES)
    spec = P(None, *AXES)
    return jax.shard_map(
        functools.partial(per_device, shape),
        mesh=mesh,
        in_specs=(spec, spec),
        out_specs=(spec, spec, P()),
        check_vma=False,
    )
```

```python
import functools

import jax
import jax.numpy as jnp
import numpy as np
from jax import lax
from jax.experimental import pallas as pl
from jax.experimental.pallas import tpu as pltpu
from jax.sharding import PartitionSpec as P

MESH = pl.DeviceIdType.MESH
STEPS = 3
AXES = ("gx", "gy", "gz")

FLOW_SET = [
    (0, 0, 0),
    (1, 0, 0),
    (-1, 0, 0),
    (0, 1, 0),
    (0, -1, 0),
    (0, 0, 1),
    (0, 0, -1),
    (1, 1, 0),
    (-1, -1, 0),
    (1, -1, 0),
    (-1, 1, 0),
    (1, 0, 1),
    (-1, 0, -1),
    (1, 0, -1),
    (-1, 0, 1),
    (0, 1, 1),
    (0, -1, -1),
    (0, 1, -1),
    (0, -1, 1),
]
LATTICE = FLOW_SET + FLOW_SET[:7]
FLOWS = len(FLOW_SET)
POPS = len(LATTICE)
TAU_FLOW = 0.6
TAU_HEAT = 0.7
GRAVITY_LIFT = 0.01
HOT_WALL = 0.5
COLD_WALL = -0.5
DIFFUSIVITY = (TAU_HEAT - 0.5) / 4.0


def opposite(q):
    c = tuple(-v for v in LATTICE[q])
    return FLOW_SET.index(c) + (FLOWS if q >= FLOWS else 0)


def movers(axis, sign):
    return [q for q in range(POPS) if LATTICE[q][axis] == sign]


XP, XM = movers(0, 1), movers(0, -1)
YM = {1: movers(1, 1), -1: movers(1, -1)}
ZM = {1: movers(2, 1), -1: movers(2, -1)}
FACE = len(XP)
ORDER = XP + XM + [q for q in range(POPS) if LATTICE[q][0] == 0]
POS = {q: i for i, q in enumerate(ORDER)}
XY = [q for q in range(FLOWS) if LATTICE[q][0] != 0 and LATTICE[q][1] != 0]
XZ = [q for q in range(FLOWS) if LATTICE[q][0] != 0 and LATTICE[q][2] != 0]
LANE0 = 8


def messages():
    out = [("xz", q, LATTICE[q]) for q in XZ]
    out += [("xy", q, LATTICE[q]) for q in XY]
    out += [("x", 1, (1, 0, 0)), ("x", -1, (-1, 0, 0))]
    out += [("yz", (cz, cy), (0, cy, cz)) for cz in (1, -1) for cy in (1, -1)]
    out += [("z", cz, (0, 0, cz)) for cz in (1, -1)]
    out += [("y", 1, (0, 1, 0)), ("y", -1, (0, -1, 0))]
    return out


MESSAGES = messages()
EDGE = {m[:2]: i for i, m in enumerate(m for m in MESSAGES if m[0] in ("xy", "yz"))}
END_PLANES = ("x", "xy", "xz")
ALL_PLANES = ("y", "z", "yz")


def collide(f):
    s, d = {}, {}
    for q in range(1, FLOWS, 2):
        s[q] = f[q] + f[q + 1]
        d[q] = f[q] - f[q + 1]
    rho = (((s[1] + s[3]) + (s[5] + s[7])) + ((s[9] + s[11]) + (s[13] + s[15]))) + (s[17] + f[0])
    jx = (d[1] + d[7]) + (d[9] + d[11]) + d[13]
    jy = (d[3] + d[7]) + (d[15] + d[17]) - d[9]
    jz = (d[5] + d[11]) + (d[15] - d[13]) - d[17]
    g = [f[FLOWS + i] for i in range(7)]
    warmth = ((g[0] + g[1]) + (g[2] + g[3])) + ((g[4] + g[5]) + g[6])
    force = GRAVITY_LIFT * rho * warmth
    inv = 1.0 / rho
    ux = jx * inv
    uy = jy * inv
    uz = (jz + 0.5 * force) * inv

    w2 = 1.0 / 36.0
    keep = 1.0 - 1.0 / TAU_FLOW
    r = (w2 / TAU_FLOW) * rho
    sf = (w2 * (1.0 - 0.5 / TAU_FLOW)) * force
    r3 = 3.0 * r
    rx, ry, rz = r3 * ux, r3 * uy, r3 * uz
    sf3 = 3.0 * sf
    ax, ay, az = rx, ry, rz + sf3
    bx, by, bz = 1.5 * rx, 1.5 * ry, 1.5 * rz + 3.0 * sf3
    qx, qy, qz = ux * bx, uy * by, uz * bz
    usq = rx * ux + ry * uy + rz * uz
    base = r - 0.5 * usq - sf3 * uz
    cxy = ux * by + uy * bx
    cxz = ux * bz + uz * bx
    cyz = uy * bz + uz * by

    out = {0: keep * f[0] + 12.0 * base}

    def pair(q, even, odd):
        out[q] = keep * f[q] + (even + odd)
        out[q + 1] = keep * f[q + 1] + (even - odd)

    pair(1, 2.0 * (base + qx), 2.0 * ax)
    pair(3, 2.0 * (base + qy), 2.0 * ay)
    pair(5, 2.0 * (base + qz), 2.0 * az)
    exy = base + (qx + qy)
    exz = base + (qx + qz)
    eyz = base + (qy + qz)
    pair(7, exy + cxy, ax + ay)
    pair(9, exy - cxy, ax - ay)
    pair(11, exz + cxz, ax + az)
    pair(13, exz - cxz, ax - az)
    pair(15, eyz + cyz, ay + az)
    pair(17, eyz - cyz, ay - az)

    keep_heat = 1.0 - 1.0 / TAU_HEAT
    t8 = (0.125 / TAU_HEAT) * warmth
    t2 = 4.0 * t8
    out[FLOWS] = keep_heat * g[0] + 2.0 * t8
    for i, u in ((1, ux), (3, uy), (5, uz)):
        odd = t2 * u
        out[FLOWS + i] = keep_heat * g[i] + (t8 + odd)
        out[FLOWS + i + 1] = keep_heat * g[i + 1] + (t8 - odd)
    return out


def flux(f):
    total = lambda values: functools.reduce(lambda a, b: a + b, values)
    rho = total([f[q] for q in range(FLOWS)])
    jz = total([f[q] for q in range(FLOWS) if LATTICE[q][2] == 1]) - total(
        [f[q] for q in range(FLOWS) if LATTICE[q][2] == -1]
    )
    warmth = total([f[q] for q in range(FLOWS, POPS)])
    force = GRAVITY_LIFT * rho * warmth
    return (jz + 0.5 * force) / rho * warmth


def kernel(
    shape,
    sizes,
    flow_in,
    heat_in,
    flow_out,
    heat_out,
    total,
    held,
    post,
    ysend,
    yrecv,
    zsend,
    zrecv,
    zdiag,
    edge_send,
    edge_recv,
    part,
    parts,
    in_sem,
    send_sem,
    recv_sem,
    part_send,
    part_recv,
    total_send,
    total_recv,
):
    nx, ny, nz = shape
    planes, rows, lanes = sizes
    me = tuple(lax.axis_index(a) for a in AXES)
    count = nx * ny * nz
    group = ny * nz
    lines = nx - nx // 4
    my_index = me[0] * group + me[1] * nz + me[2]
    is_root = me[0] < lines

    def at(off):
        return tuple(m if d == 0 else lax.rem(m + (d % n), n) for m, d, n in zip(me, off, shape))

    offsets = [off for off in np.ndindex(3, 3, 3) if off != (1, 1, 1)]
    offsets = [tuple(d - 1 for d in off) for off in offsets if 1 in off]
    offsets.sort(key=lambda off: -2 * abs(off[0]) - abs(off[2]))
    barrier = pltpu.get_barrier_semaphore()
    for off in offsets:
        pl.semaphore_signal(barrier, inc=1, device_id=at(off), device_id_type=MESH)

    inner, ends = range(1, planes - 1), (0, planes - 1)
    blocks = [(0, 1), (planes - 1, 1), (1, planes - 2)]
    loads = []
    for i, (x, n) in enumerate(blocks):
        some = pl.ds(x * rows, n * rows)
        for j, (ref, low, n) in enumerate(((flow_in, 0, FLOWS), (heat_in, FLOWS, 7))):
            loads.append(
                pltpu.make_async_copy(ref.at[:, some], held.at[pl.ds(low, n), some], in_sem.at[2 * i + j])
            )
    for c in loads:
        c.start()

    @pl.when(is_root)
    def _():
        for d in range(1, nx):
            pl.semaphore_signal(barrier, inc=1, device_id=at((d, 0, 0)), device_id_type=MESH)

    lane = lax.broadcasted_iota(jnp.int32, (rows, lanes), 1)
    row = lax.broadcasted_iota(jnp.int32, (rows, lanes), 0)
    is_bottom = me[2] == 0
    is_top = me[2] == nz - 1
    end_lane = {1: lane == 0, -1: lane == lanes - 1}
    wall = {1: jnp.logical_and(end_lane[1], is_bottom), -1: jnp.logical_and(end_lane[-1], is_top)}
    end_row = {1: row == 0, -1: row == rows - 1}
    far_row = {1: rows - 1, -1: 0}
    side = {1: 0, -1: 1}

    def turn(v, c, axis):
        n = rows if axis == 0 else lanes
        return pltpu.roll(v, 1 if c == 1 else n - 1, axis)

    def plane(x):
        return pl.ds((x + 1) * rows, rows)

    def keep(s, x, out, packed):
        if x in ends:
            cx = 1 if x else -1
            for q in XY:
                if LATTICE[q][0] == cx:
                    far = far_row[LATTICE[q][1]]
                    edge_send[s, EDGE["xy", q]] = out[q][far : far + 1, :]
        for q in range(POPS):
            post[s, POS[q], plane(x), :] = out[q]
        for cz in (1, -1):
            for j, q in enumerate(ZM[cz]):
                k = LANE0 + j * planes + x
                packed[cz] = jnp.where(lane == k, pltpu.roll(out[q], k + (1 if cz == 1 else 0), 1), packed[cz])

    def crew(end, dz):
        return (0 if end else 3) + dz + 1

    def copy(s, m):
        kind, slot, off = MESSAGES[m]
        if kind == "x":
            some = pl.ds(0 if slot == 1 else FACE, FACE)
            src, dst = (planes - 1, -1) if slot == 1 else (0, planes)
            src, dst = post.at[s, some, plane(src)], post.at[s, some, plane(dst)]
        elif kind == "y":
            src, dst = ysend.at[s, side[slot]], yrecv.at[s, side[slot]]
        elif kind == "z":
            src, dst = zsend.at[s, side[slot]], zrecv.at[s, side[slot]]
        elif kind == "xz":
            src = post.at[s, POS[slot], plane(planes - 1 if off[0] == 1 else 0)]
            dst = zdiag.at[s, XZ.index(slot)]
        else:
            src, dst = edge_send.at[s, EDGE[kind, slot]], edge_recv.at[s, EDGE[kind, slot]]
        return pltpu.make_async_remote_copy(
            src_ref=src,
            dst_ref=dst,
            send_sem=send_sem.at[s, crew(kind in END_PLANES, off[2])],
            recv_sem=recv_sem.at[s, crew(kind in END_PLANES, off[2])],
            device_id=at(off),
            device_id_type=MESH,
        )

    def of_kind(kinds, dz):
        return [m for m, (kind, _, off) in enumerate(MESSAGES) if kind in kinds and off[2] == dz]

    def each(act, up, down):
        for dz, when in ((1, up), (-1, down)):

            @pl.when(when)
            def _():
                act(dz)

        act(0)

    def start(s, kinds):
        def act(dz):
            for m in of_kind(kinds, dz):
                copy(s, m).start()

        each(act, jnp.logical_not(is_top), jnp.logical_not(is_bottom))

    def bytes_of(s, kinds, dz):
        size = {"x": FACE * rows, "y": FACE * planes, "z": rows, "xz": rows, "xy": 1, "yz": 1}
        some = parts.at[pl.ds(0, sum(size[MESSAGES[m][0]] for m in of_kind(kinds, dz)))]
        return pltpu.make_async_remote_copy(
            src_ref=some,
            dst_ref=some,
            send_sem=send_sem.at[s, crew(kinds == END_PLANES, dz)],
            recv_sem=recv_sem.at[s, crew(kinds == END_PLANES, dz)],
            device_id=at((1, 0, 0)),
            device_id_type=MESH,
        )

    def receive(s, kinds):
        each(lambda dz: bytes_of(s, kinds, dz).wait_recv(), jnp.logical_not(is_bottom), jnp.logical_not(is_top))

    def drain(s, kinds):
        each(lambda dz: bytes_of(s, kinds, dz).wait_send(), jnp.logical_not(is_top), jnp.logical_not(is_bottom))

    def pack(s, packed):
        for cy in (1, -1):
            first = rows + far_row[cy]
            for j, q in enumerate(YM[cy]):
                ysend[s, side[cy], j] = post[s, POS[q], pl.ds(first, planes, stride=rows), :]
        for cz in (1, -1):
            zsend[s, side[cz]] = packed[cz]
            for cy in (1, -1):
                far = far_row[cy]
                edge_send[s, EDGE["yz", (cz, cy)]] = packed[cz][far : far + 1, :]

    def z_faces(s):
        tiles = {}
        for cz in (1, -1):
            own = zrecv[s, side[cz]]
            tiles[cz, 0] = own
            for cy in (1, -1):
                other = jnp.broadcast_to(edge_recv[s, EDGE["yz", (cz, cy)]], (rows, lanes))
                tiles[cz, cy] = jnp.where(end_row[cy], other, turn(own, cy, 0))
        return tiles

    def stream(s, x, tiles):
        f = {}
        for q in range(POPS):
            cx, cy, cz = LATTICE[q]
            v = post[s, POS[q], plane(x - cx), :]
            inside = 0 <= x - cx < planes
            if cy:
                if inside:
                    edge = yrecv[s, side[cy], YM[cy].index(q), pl.ds(x - cx, 1), :]
                else:
                    edge = edge_recv[s, EDGE["xy", q]]
                v = jnp.where(end_row[cy], jnp.broadcast_to(edge, (rows, lanes)), turn(v, cy, 0))
            if cz:
                if inside:
                    k = LANE0 + ZM[cz].index(q) * planes + x - cx
                    edge = pltpu.roll(tiles[cz, cy], (lanes if cz == 1 else lanes - 1) - k, 1)
                else:
                    edge = turn(zdiag[s, XZ.index(q)], cz, 1)
                back = post[s, POS[opposite(q)], plane(x), :]
                if q >= FLOWS:
                    back = 0.25 * (HOT_WALL if cz == 1 else COLD_WALL) - back
                v = jnp.where(wall[cz], back, jnp.where(end_lane[cz], edge, turn(v, cz, 1)))
            f[q] = v
        return f

    blank = jnp.zeros((rows, lanes), jnp.float32)

    def first(x, packed):
        keep(0, x, collide({q: held[q, pl.ds(x * rows, rows), :] for q in range(POPS)}), packed)

    packed = {1: blank, -1: blank}
    for c in loads[:4]:
        c.wait()
    for x in ends:
        first(x, packed)
    pl.semaphore_wait(barrier, len(offsets) + lines - is_root.astype(jnp.int32))
    start(0, END_PLANES)
    for c in loads[4:]:
        c.wait()
    for x in inner:
        first(x, packed)
    pack(0, packed)
    start(0, ALL_PLANES)

    for s in range(1, STEPS):
        packed = {1: blank, -1: blank}
        receive(s - 1, ALL_PLANES)
        tiles = z_faces(s - 1)
        for x in inner:
            keep(s, x, collide(stream(s - 1, x, tiles)), packed)
        receive(s - 1, END_PLANES)
        for x in ends:
            keep(s, x, collide(stream(s - 1, x, tiles)), packed)
        start(s, END_PLANES)
        pack(s, packed)
        start(s, ALL_PLANES)

    def last(x, tiles):
        f = stream(STEPS - 1, x, tiles)
        for q in range(FLOWS):
            flow_out[q, pl.ds(x * rows, rows), :] = f[q]
        for q in range(FLOWS, POPS):
            heat_out[q - FLOWS, pl.ds(x * rows, rows), :] = f[q]
        return flux(f)

    receive(STEPS - 1, ALL_PLANES)
    tiles = z_faces(STEPS - 1)
    acc = blank
    for x in inner:
        acc = acc + last(x, tiles)
    receive(STEPS - 1, END_PLANES)
    for x in ends:
        acc = acc + last(x, tiles)

    mine = jnp.sum(acc, axis=0, keepdims=True)
    part[0] = mine
    parts[my_index] = mine
    seat = lax.rem(my_index, group)

    def to_root(x, d):
        return pltpu.make_async_remote_copy(
            src_ref=part.at[0],
            dst_ref=parts.at[my_index],
            send_sem=part_send.at[0],
            recv_sem=part_recv.at[0],
            device_id=x * group + lax.rem(seat + d, group),
            device_id_type=pl.DeviceIdType.LOGICAL,
        )

    for x in range(lines):

        @pl.when(me[0] != x)
        def _():
            to_root(x, 0).start()

        for d in range(1, group):
            to_root(x, d).start()

    serves = jnp.logical_and(me[0] >= nx // 2, is_root)
    served = [nx + nx // 2 - 1 - me[0]]

    def to_served(i):
        return pltpu.make_async_remote_copy(
            src_ref=total.at[0],
            dst_ref=total.at[0],
            send_sem=total_send.at[i],
            recv_sem=total_recv.at[0],
            device_id=(served[i], me[1], me[2]),
            device_id_type=MESH,
        )

    def whole(n, k):
        some = parts.at[pl.ds(0, n)]
        return pltpu.make_async_remote_copy(
            src_ref=some,
            dst_ref=some,
            send_sem=part_send.at[k],
            recv_sem=part_recv.at[0],
            device_id=0,
            device_id_type=pl.DeviceIdType.LOGICAL,
        )

    for s in range(STEPS):
        drain(s, END_PLANES)
        drain(s, ALL_PLANES)

    @pl.when(is_root)
    def _():
        whole(lines * group - 1, 0).wait_send()

    @pl.when(jnp.logical_not(is_root))
    def _():
        whole(lines * group, 0).wait_send()

    @pl.when(is_root)
    def _():
        whole(count - 1, 0).wait_recv()
        sums = [parts[i] for i in range(8)]
        for i in range(8, count):
            sums[i % 8] = sums[i % 8] + parts[i]
        total[0] = ((sums[0] + sums[1]) + (sums[2] + sums[3])) + ((sums[4] + sums[5]) + (sums[6] + sums[7]))

        @pl.when(serves)
        def _():
            to_served(0).start()

    @pl.when(jnp.logical_not(is_root))
    def _():
        to_served(0).wait_recv()

    @pl.when(serves)
    def _():
        to_served(0).wait_send()


def write_out(scale, flow, heat, total, flow_out, heat_out, nusselt, value, sem):
    copies = [
        pltpu.make_async_copy(flow, flow_out, sem.at[0]),
        pltpu.make_async_copy(heat, heat_out, sem.at[1]),
    ]
    for c in copies:
        c.start()
    value[...] = 1.0 + scale * jnp.sum(total[0], axis=1, keepdims=True)
    copies.append(pltpu.make_async_copy(value, nusselt, sem.at[2]))
    copies[2].start()
    for c in copies:
        c.wait()


def per_device(shape, flow_pops, heat_pops):
    nx, ny, nz = shape
    _, planes, rows, lanes = flow_pops.shape
    flat = (planes * rows, lanes)
    dma = pltpu.SemaphoreType.DMA
    tile = (rows, lanes)
    vmem = lambda *dims: pltpu.VMEM(dims, jnp.float32)
    anywhere = pl.BlockSpec(memory_space=pl.ANY)
    in_vmem = pl.BlockSpec(memory_space=pltpu.VMEM)
    state = pl.pallas_call(
        functools.partial(kernel, shape, (planes, rows, lanes)),
        out_shape=(
            vmem(FLOWS, *flat),
            vmem(7, *flat),
            vmem(1, 1, lanes),
        ),
        in_specs=[anywhere] * 2,
        out_specs=(in_vmem,) * 3,
        scratch_shapes=[
            vmem(POPS, *flat),
            vmem(STEPS, POPS, (planes + 2) * rows, lanes),
            vmem(STEPS, 2, FACE, *tile),
            vmem(STEPS, 2, FACE, *tile),
            vmem(STEPS, 2, *tile),
            vmem(STEPS, 2, *tile),
            vmem(STEPS, len(XZ), *tile),
            vmem(STEPS, len(EDGE), 1, lanes),
            vmem(STEPS, len(EDGE), 1, lanes),
            vmem(1, 1, lanes),
            vmem(max(nx * ny * nz, 128), 1, lanes),
            dma((6,)),
            dma((STEPS, 6)),
            dma((STEPS, 6)),
            dma((1,)),
            dma((1,)),
            dma((1,)),
            dma((1,)),
        ],
        compiler_params=pltpu.CompilerParams(collective_id=0, has_side_effects=True),
        name="lattice_steps",
    )(flow_pops.reshape((FLOWS,) + flat), heat_pops.reshape((7,) + flat))
    cells = nx * ny * nz * planes * rows * lanes
    scale = nz * lanes / (DIFFUSIVITY * (HOT_WALL - COLD_WALL)) / cells
    flow, heat, nusselt = pl.pallas_call(
        functools.partial(write_out, scale),
        out_shape=(
            jax.ShapeDtypeStruct((FLOWS,) + flat, jnp.float32),
            jax.ShapeDtypeStruct((7,) + flat, jnp.float32),
            jax.ShapeDtypeStruct((1, 1), jnp.float32),
        ),
        in_specs=[in_vmem] * 3,
        out_specs=(anywhere,) * 3,
        scratch_shapes=[vmem(1, 1), dma((3,))],
        name="write_out",
    )(*(pltpu.with_memory_space_constraint(a, pltpu.VMEM) for a in state))
    return flow.reshape(flow_pops.shape), heat.reshape(heat_pops.shape), nusselt.reshape(())


def solution(mesh):
    shape = tuple(mesh.shape[a] for a in AXES)
    spec = P(None, *AXES)
    return jax.shard_map(
        functools.partial(per_device, shape),
        mesh=mesh,
        in_specs=(spec, spec),
        out_specs=(spec, spec, P()),
        check_vma=False,
    )
```

```python
import functools

import jax
import jax.numpy as jnp
import numpy as np
from jax import lax
from jax.experimental import pallas as pl
from jax.experimental.pallas import tpu as pltpu
from jax.sharding import PartitionSpec as P

MESH = pl.DeviceIdType.MESH
STEPS = 3
AXES = ("gx", "gy", "gz")

FLOW_SET = [
    (0, 0, 0),
    (1, 0, 0),
    (-1, 0, 0),
    (0, 1, 0),
    (0, -1, 0),
    (0, 0, 1),
    (0, 0, -1),
    (1, 1, 0),
    (-1, -1, 0),
    (1, -1, 0),
    (-1, 1, 0),
    (1, 0, 1),
    (-1, 0, -1),
    (1, 0, -1),
    (-1, 0, 1),
    (0, 1, 1),
    (0, -1, -1),
    (0, 1, -1),
    (0, -1, 1),
]
LATTICE = FLOW_SET + FLOW_SET[:7]
FLOWS = len(FLOW_SET)
POPS = len(LATTICE)
TAU_FLOW = 0.6
TAU_HEAT = 0.7
GRAVITY_LIFT = 0.01
HOT_WALL = 0.5
COLD_WALL = -0.5
DIFFUSIVITY = (TAU_HEAT - 0.5) / 4.0


def opposite(q):
    c = tuple(-v for v in LATTICE[q])
    return FLOW_SET.index(c) + (FLOWS if q >= FLOWS else 0)


def movers(axis, sign):
    return [q for q in range(POPS) if LATTICE[q][axis] == sign]


XP, XM = movers(0, 1), movers(0, -1)
YM = {1: movers(1, 1), -1: movers(1, -1)}
ZM = {1: movers(2, 1), -1: movers(2, -1)}
FACE = len(XP)
ORDER = XP + XM + [q for q in range(POPS) if LATTICE[q][0] == 0]
POS = {q: i for i, q in enumerate(ORDER)}
XY = [q for q in range(FLOWS) if LATTICE[q][0] != 0 and LATTICE[q][1] != 0]
XZ = [q for q in range(FLOWS) if LATTICE[q][0] != 0 and LATTICE[q][2] != 0]
LANE0 = 8


def messages():
    out = [("xz", q, LATTICE[q]) for q in XZ]
    out += [("xy", q, LATTICE[q]) for q in XY]
    out += [("x", 1, (1, 0, 0)), ("x", -1, (-1, 0, 0))]
    out += [("yz", (cz, cy), (0, cy, cz)) for cz in (1, -1) for cy in (1, -1)]
    out += [("z", cz, (0, 0, cz)) for cz in (1, -1)]
    out += [("y", 1, (0, 1, 0)), ("y", -1, (0, -1, 0))]
    return out


MESSAGES = messages()
EDGE = {m[:2]: i for i, m in enumerate(m for m in MESSAGES if m[0] in ("xy", "yz"))}
END_PLANES = ("x", "xy", "xz")
ALL_PLANES = ("y", "z", "yz")


def collide(f):
    s, d = {}, {}
    for q in range(1, FLOWS, 2):
        s[q] = f[q] + f[q + 1]
        d[q] = f[q] - f[q + 1]
    rho = (((s[1] + s[3]) + (s[5] + s[7])) + ((s[9] + s[11]) + (s[13] + s[15]))) + (s[17] + f[0])
    jx = (d[1] + d[7]) + (d[9] + d[11]) + d[13]
    jy = (d[3] + d[7]) + (d[15] + d[17]) - d[9]
    jz = (d[5] + d[11]) + (d[15] - d[13]) - d[17]
    g = [f[FLOWS + i] for i in range(7)]
    warmth = ((g[0] + g[1]) + (g[2] + g[3])) + ((g[4] + g[5]) + g[6])
    force = GRAVITY_LIFT * rho * warmth
    inv = 1.0 / rho
    ux = jx * inv
    uy = jy * inv
    uz = (jz + 0.5 * force) * inv

    w2 = 1.0 / 36.0
    keep = 1.0 - 1.0 / TAU_FLOW
    r = (w2 / TAU_FLOW) * rho
    sf = (w2 * (1.0 - 0.5 / TAU_FLOW)) * force
    r3 = 3.0 * r
    rx, ry, rz = r3 * ux, r3 * uy, r3 * uz
    sf3 = 3.0 * sf
    ax, ay, az = rx, ry, rz + sf3
    bx, by, bz = 1.5 * rx, 1.5 * ry, 1.5 * rz + 3.0 * sf3
    qx, qy, qz = ux * bx, uy * by, uz * bz
    usq = rx * ux + ry * uy + rz * uz
    base = r - 0.5 * usq - sf3 * uz
    cxy = ux * by + uy * bx
    cxz = ux * bz + uz * bx
    cyz = uy * bz + uz * by

    out = {0: keep * f[0] + 12.0 * base}

    def pair(q, even, odd):
        out[q] = keep * f[q] + (even + odd)
        out[q + 1] = keep * f[q + 1] + (even - odd)

    pair(1, 2.0 * (base + qx), 2.0 * ax)
    pair(3, 2.0 * (base + qy), 2.0 * ay)
    pair(5, 2.0 * (base + qz), 2.0 * az)
    exy = base + (qx + qy)
    exz = base + (qx + qz)
    eyz = base + (qy + qz)
    pair(7, exy + cxy, ax + ay)
    pair(9, exy - cxy, ax - ay)
    pair(11, exz + cxz, ax + az)
    pair(13, exz - cxz, ax - az)
    pair(15, eyz + cyz, ay + az)
    pair(17, eyz - cyz, ay - az)

    keep_heat = 1.0 - 1.0 / TAU_HEAT
    t8 = (0.125 / TAU_HEAT) * warmth
    t2 = 4.0 * t8
    out[FLOWS] = keep_heat * g[0] + 2.0 * t8
    for i, u in ((1, ux), (3, uy), (5, uz)):
        odd = t2 * u
        out[FLOWS + i] = keep_heat * g[i] + (t8 + odd)
        out[FLOWS + i + 1] = keep_heat * g[i + 1] + (t8 - odd)
    return out


def flux(f):
    total = lambda values: functools.reduce(lambda a, b: a + b, values)
    rho = total([f[q] for q in range(FLOWS)])
    jz = total([f[q] for q in range(FLOWS) if LATTICE[q][2] == 1]) - total(
        [f[q] for q in range(FLOWS) if LATTICE[q][2] == -1]
    )
    warmth = total([f[q] for q in range(FLOWS, POPS)])
    force = GRAVITY_LIFT * rho * warmth
    return (jz + 0.5 * force) / rho * warmth


def kernel(
    shape,
    sizes,
    flow_in,
    heat_in,
    flow_out,
    heat_out,
    total,
    held,
    post,
    ysend,
    yrecv,
    zsend,
    zrecv,
    zdiag,
    edge_send,
    edge_recv,
    part,
    parts,
    in_sem,
    send_sem,
    recv_sem,
    part_send,
    part_recv,
    total_send,
    total_recv,
):
    nx, ny, nz = shape
    planes, rows, lanes = sizes
    me = tuple(lax.axis_index(a) for a in AXES)
    count = nx * ny * nz
    group = ny * nz
    lines = nx - nx // 4
    my_index = me[0] * group + me[1] * nz + me[2]
    is_root = me[0] < lines

    def at(off):
        return tuple(m if d == 0 else lax.rem(m + (d % n), n) for m, d, n in zip(me, off, shape))

    offsets = [off for off in np.ndindex(3, 3, 3) if off != (1, 1, 1)]
    offsets = [tuple(d - 1 for d in off) for off in offsets if 1 in off]
    offsets.sort(key=lambda off: -2 * abs(off[0]) - abs(off[2]))
    barrier = pltpu.get_barrier_semaphore()
    for off in offsets:
        pl.semaphore_signal(barrier, inc=1, device_id=at(off), device_id_type=MESH)

    inner, ends = range(1, planes - 1), (0, planes - 1)
    blocks = [(0, 1), (planes - 1, 1), (1, planes - 2)]
    loads = []
    for i, (x, n) in enumerate(blocks):
        some = pl.ds(x * rows, n * rows)
        for j, (ref, low, n) in enumerate(((flow_in, 0, FLOWS), (heat_in, FLOWS, 7))):
            loads.append(
                pltpu.make_async_copy(ref.at[:, some], held.at[pl.ds(low, n), some], in_sem.at[2 * i + j])
            )
    for c in loads:
        c.start()

    @pl.when(is_root)
    def _():
        for d in range(1, nx):
            pl.semaphore_signal(barrier, inc=1, device_id=at((d, 0, 0)), device_id_type=MESH)

    lane = lax.broadcasted_iota(jnp.int32, (rows, lanes), 1)
    row = lax.broadcasted_iota(jnp.int32, (rows, lanes), 0)
    is_bottom = me[2] == 0
    is_top = me[2] == nz - 1
    end_lane = {1: lane == 0, -1: lane == lanes - 1}
    wall = {1: jnp.logical_and(end_lane[1], is_bottom), -1: jnp.logical_and(end_lane[-1], is_top)}
    end_row = {1: row == 0, -1: row == rows - 1}
    far_row = {1: rows - 1, -1: 0}
    side = {1: 0, -1: 1}

    def turn(v, c, axis):
        n = rows if axis == 0 else lanes
        return pltpu.roll(v, 1 if c == 1 else n - 1, axis)

    def plane(x):
        return pl.ds((x + 1) * rows, rows)

    def keep(s, x, out, packed):
        if x in ends:
            cx = 1 if x else -1
            for q in XY:
                if LATTICE[q][0] == cx:
                    far = far_row[LATTICE[q][1]]
                    edge_send[s, EDGE["xy", q]] = out[q][far : far + 1, :]
        for q in range(POPS):
            post[s, POS[q], plane(x), :] = out[q]
        for cz in (1, -1):
            for j, q in enumerate(ZM[cz]):
                k = LANE0 + j * planes + x
                packed[cz] = jnp.where(lane == k, pltpu.roll(out[q], k + (1 if cz == 1 else 0), 1), packed[cz])

    def crew(end, dz):
        return (0 if end else 3) + dz + 1

    def copy(s, m):
        kind, slot, off = MESSAGES[m]
        if kind == "x":
            some = pl.ds(0 if slot == 1 else FACE, FACE)
            src, dst = (planes - 1, -1) if slot == 1 else (0, planes)
            src, dst = post.at[s, some, plane(src)], post.at[s, some, plane(dst)]
        elif kind == "y":
            src, dst = ysend.at[s, side[slot]], yrecv.at[s, side[slot]]
        elif kind == "z":
            src, dst = zsend.at[s, side[slot]], zrecv.at[s, side[slot]]
        elif kind == "xz":
            src = post.at[s, POS[slot], plane(planes - 1 if off[0] == 1 else 0)]
            dst = zdiag.at[s, XZ.index(slot)]
        else:
            src, dst = edge_send.at[s, EDGE[kind, slot]], edge_recv.at[s, EDGE[kind, slot]]
        return pltpu.make_async_remote_copy(
            src_ref=src,
            dst_ref=dst,
            send_sem=send_sem.at[s, crew(kind in END_PLANES, off[2])],
            recv_sem=recv_sem.at[s, crew(kind in END_PLANES, off[2])],
            device_id=at(off),
            device_id_type=MESH,
        )

    def of_kind(kinds, dz):
        return [m for m, (kind, _, off) in enumerate(MESSAGES) if kind in kinds and off[2] == dz]

    def each(act, up, down):
        for dz, when in ((1, up), (-1, down)):

            @pl.when(when)
            def _():
                act(dz)

        act(0)

    def start(s, kinds):
        def act(dz):
            for m in of_kind(kinds, dz):
                copy(s, m).start()

        each(act, jnp.logical_not(is_top), jnp.logical_not(is_bottom))

    def bytes_of(s, kinds, dz):
        size = {"x": FACE * rows, "y": FACE * planes, "z": rows, "xz": rows, "xy": 1, "yz": 1}
        some = parts.at[pl.ds(0, sum(size[MESSAGES[m][0]] for m in of_kind(kinds, dz)))]
        return pltpu.make_async_remote_copy(
            src_ref=some,
            dst_ref=some,
            send_sem=send_sem.at[s, crew(kinds == END_PLANES, dz)],
            recv_sem=recv_sem.at[s, crew(kinds == END_PLANES, dz)],
            device_id=at((1, 0, 0)),
            device_id_type=MESH,
        )

    def receive(s, kinds):
        each(lambda dz: bytes_of(s, kinds, dz).wait_recv(), jnp.logical_not(is_bottom), jnp.logical_not(is_top))

    def drain(s, kinds):
        each(lambda dz: bytes_of(s, kinds, dz).wait_send(), jnp.logical_not(is_top), jnp.logical_not(is_bottom))

    def pack(s, packed):
        for cy in (1, -1):
            first = rows + far_row[cy]
            for j, q in enumerate(YM[cy]):
                ysend[s, side[cy], j] = post[s, POS[q], pl.ds(first, planes, stride=rows), :]
        for cz in (1, -1):
            zsend[s, side[cz]] = packed[cz]
            for cy in (1, -1):
                far = far_row[cy]
                edge_send[s, EDGE["yz", (cz, cy)]] = packed[cz][far : far + 1, :]

    def z_faces(s):
        tiles = {}
        for cz in (1, -1):
            own = zrecv[s, side[cz]]
            tiles[cz, 0] = own
            for cy in (1, -1):
                other = jnp.broadcast_to(edge_recv[s, EDGE["yz", (cz, cy)]], (rows, lanes))
                tiles[cz, cy] = jnp.where(end_row[cy], other, turn(own, cy, 0))
        return tiles

    def stream(s, x, tiles):
        f = {}
        for q in range(POPS):
            cx, cy, cz = LATTICE[q]
            v = post[s, POS[q], plane(x - cx), :]
            inside = 0 <= x - cx < planes
            if cy:
                if inside:
                    edge = yrecv[s, side[cy], YM[cy].index(q), pl.ds(x - cx, 1), :]
                else:
                    edge = edge_recv[s, EDGE["xy", q]]
                v = jnp.where(end_row[cy], jnp.broadcast_to(edge, (rows, lanes)), turn(v, cy, 0))
            if cz:
                if inside:
                    k = LANE0 + ZM[cz].index(q) * planes + x - cx
                    edge = pltpu.roll(tiles[cz, cy], (lanes if cz == 1 else lanes - 1) - k, 1)
                else:
                    edge = turn(zdiag[s, XZ.index(q)], cz, 1)
                back = post[s, POS[opposite(q)], plane(x), :]
                if q >= FLOWS:
                    back = 0.25 * (HOT_WALL if cz == 1 else COLD_WALL) - back
                v = jnp.where(wall[cz], back, jnp.where(end_lane[cz], edge, turn(v, cz, 1)))
            f[q] = v
        return f

    blank = jnp.zeros((rows, lanes), jnp.float32)

    def first(x, packed):
        keep(0, x, collide({q: held[q, pl.ds(x * rows, rows), :] for q in range(POPS)}), packed)

    packed = {1: blank, -1: blank}
    for c in loads[:4]:
        c.wait()
    for x in ends:
        first(x, packed)
    for c in loads[4:]:
        c.wait()
    for x in inner:
        first(x, packed)
    pack(0, packed)
    pl.semaphore_wait(barrier, len(offsets) + lines - is_root.astype(jnp.int32))
    start(0, END_PLANES)
    start(0, ALL_PLANES)

    for s in range(1, STEPS):
        packed = {1: blank, -1: blank}
        receive(s - 1, ALL_PLANES)
        tiles = z_faces(s - 1)
        for x in inner:
            keep(s, x, collide(stream(s - 1, x, tiles)), packed)
        receive(s - 1, END_PLANES)
        for x in ends:
            keep(s, x, collide(stream(s - 1, x, tiles)), packed)
        start(s, END_PLANES)
        pack(s, packed)
        start(s, ALL_PLANES)

    def last(x, tiles):
        f = stream(STEPS - 1, x, tiles)
        for q in range(FLOWS):
            flow_out[q, pl.ds(x * rows, rows), :] = f[q]
        for q in range(FLOWS, POPS):
            heat_out[q - FLOWS, pl.ds(x * rows, rows), :] = f[q]
        return flux(f)

    receive(STEPS - 1, ALL_PLANES)
    tiles = z_faces(STEPS - 1)
    acc = blank
    for x in inner:
        acc = acc + last(x, tiles)
    receive(STEPS - 1, END_PLANES)
    for x in ends:
        acc = acc + last(x, tiles)

    mine = jnp.sum(acc, axis=0, keepdims=True)
    part[0] = mine
    parts[my_index] = mine
    seat = lax.rem(my_index, group)

    def to_root(x, d):
        return pltpu.make_async_remote_copy(
            src_ref=part.at[0],
            dst_ref=parts.at[my_index],
            send_sem=part_send.at[0],
            recv_sem=part_recv.at[0],
            device_id=x * group + lax.rem(seat + d, group),
            device_id_type=pl.DeviceIdType.LOGICAL,
        )

    for x in range(lines):

        @pl.when(me[0] != x)
        def _():
            to_root(x, 0).start()

        for d in range(1, group):
            to_root(x, d).start()

    serves = jnp.logical_and(me[0] >= nx // 2, is_root)
    served = [nx + nx // 2 - 1 - me[0]]

    def to_served(i):
        return pltpu.make_async_remote_copy(
            src_ref=total.at[0],
            dst_ref=total.at[0],
            send_sem=total_send.at[i],
            recv_sem=total_recv.at[0],
            device_id=(served[i], me[1], me[2]),
            device_id_type=MESH,
        )

    def whole(n, k):
        some = parts.at[pl.ds(0, n)]
        return pltpu.make_async_remote_copy(
            src_ref=some,
            dst_ref=some,
            send_sem=part_send.at[k],
            recv_sem=part_recv.at[0],
            device_id=0,
            device_id_type=pl.DeviceIdType.LOGICAL,
        )

    for s in range(STEPS):
        drain(s, END_PLANES)
        drain(s, ALL_PLANES)

    @pl.when(is_root)
    def _():
        whole(lines * group - 1, 0).wait_send()

    @pl.when(jnp.logical_not(is_root))
    def _():
        whole(lines * group, 0).wait_send()

    @pl.when(is_root)
    def _():
        whole(count - 1, 0).wait_recv()
        sums = [parts[i] for i in range(8)]
        for i in range(8, count):
            sums[i % 8] = sums[i % 8] + parts[i]
        total[0] = ((sums[0] + sums[1]) + (sums[2] + sums[3])) + ((sums[4] + sums[5]) + (sums[6] + sums[7]))

        @pl.when(serves)
        def _():
            to_served(0).start()

    @pl.when(jnp.logical_not(is_root))
    def _():
        to_served(0).wait_recv()

    @pl.when(serves)
    def _():
        to_served(0).wait_send()


def write_out(scale, flow, heat, total, flow_out, heat_out, nusselt, value, sem):
    copies = [
        pltpu.make_async_copy(flow, flow_out, sem.at[0]),
        pltpu.make_async_copy(heat, heat_out, sem.at[1]),
    ]
    for c in copies:
        c.start()
    value[...] = 1.0 + scale * jnp.sum(total[0], axis=1, keepdims=True)
    copies.append(pltpu.make_async_copy(value, nusselt, sem.at[2]))
    copies[2].start()
    for c in copies:
        c.wait()


def per_device(shape, flow_pops, heat_pops):
    nx, ny, nz = shape
    _, planes, rows, lanes = flow_pops.shape
    flat = (planes * rows, lanes)
    dma = pltpu.SemaphoreType.DMA
    tile = (rows, lanes)
    vmem = lambda *dims: pltpu.VMEM(dims, jnp.float32)
    anywhere = pl.BlockSpec(memory_space=pl.ANY)
    in_vmem = pl.BlockSpec(memory_space=pltpu.VMEM)
    state = pl.pallas_call(
        functools.partial(kernel, shape, (planes, rows, lanes)),
        out_shape=(
            vmem(FLOWS, *flat),
            vmem(7, *flat),
            vmem(1, 1, lanes),
        ),
        in_specs=[anywhere] * 2,
        out_specs=(in_vmem,) * 3,
        scratch_shapes=[
            vmem(POPS, *flat),
            vmem(STEPS, POPS, (planes + 2) * rows, lanes),
            vmem(STEPS, 2, FACE, *tile),
            vmem(STEPS, 2, FACE, *tile),
            vmem(STEPS, 2, *tile),
            vmem(STEPS, 2, *tile),
            vmem(STEPS, len(XZ), *tile),
            vmem(STEPS, len(EDGE), 1, lanes),
            vmem(STEPS, len(EDGE), 1, lanes),
            vmem(1, 1, lanes),
            vmem(max(nx * ny * nz, 128), 1, lanes),
            dma((6,)),
            dma((STEPS, 6)),
            dma((STEPS, 6)),
            dma((1,)),
            dma((1,)),
            dma((1,)),
            dma((1,)),
        ],
        compiler_params=pltpu.CompilerParams(collective_id=0, has_side_effects=True),
        name="lattice_steps",
    )(flow_pops.reshape((FLOWS,) + flat), heat_pops.reshape((7,) + flat))
    cells = nx * ny * nz * planes * rows * lanes
    scale = nz * lanes / (DIFFUSIVITY * (HOT_WALL - COLD_WALL)) / cells
    flow, heat, nusselt = pl.pallas_call(
        functools.partial(write_out, scale),
        out_shape=(
            jax.ShapeDtypeStruct((FLOWS,) + flat, jnp.float32),
            jax.ShapeDtypeStruct((7,) + flat, jnp.float32),
            jax.ShapeDtypeStruct((1, 1), jnp.float32),
        ),
        in_specs=[in_vmem] * 3,
        out_specs=(anywhere,) * 3,
        scratch_shapes=[vmem(1, 1), dma((3,))],
        name="write_out",
    )(*(pltpu.with_memory_space_constraint(a, pltpu.VMEM) for a in state))
    return flow.reshape(flow_pops.shape), heat.reshape(heat_pops.shape), nusselt.reshape(())


def solution(mesh):
    shape = tuple(mesh.shape[a] for a in AXES)
    spec = P(None, *AXES)
    return jax.shard_map(
        functools.partial(per_device, shape),
        mesh=mesh,
        in_specs=(spec, spec),
        out_specs=(spec, spec, P()),
        check_vma=False,
    )
```

```python
import functools

import jax
import jax.numpy as jnp
import numpy as np
from jax import lax
from jax.experimental import pallas as pl
from jax.experimental.pallas import tpu as pltpu
from jax.sharding import PartitionSpec as P

MESH = pl.DeviceIdType.MESH
STEPS = 3
AXES = ("gx", "gy", "gz")

FLOW_SET = [
    (0, 0, 0),
    (1, 0, 0),
    (-1, 0, 0),
    (0, 1, 0),
    (0, -1, 0),
    (0, 0, 1),
    (0, 0, -1),
    (1, 1, 0),
    (-1, -1, 0),
    (1, -1, 0),
    (-1, 1, 0),
    (1, 0, 1),
    (-1, 0, -1),
    (1, 0, -1),
    (-1, 0, 1),
    (0, 1, 1),
    (0, -1, -1),
    (0, 1, -1),
    (0, -1, 1),
]
LATTICE = FLOW_SET + FLOW_SET[:7]
FLOWS = len(FLOW_SET)
POPS = len(LATTICE)
TAU_FLOW = 0.6
TAU_HEAT = 0.7
GRAVITY_LIFT = 0.01
HOT_WALL = 0.5
COLD_WALL = -0.5
DIFFUSIVITY = (TAU_HEAT - 0.5) / 4.0


def opposite(q):
    c = tuple(-v for v in LATTICE[q])
    return FLOW_SET.index(c) + (FLOWS if q >= FLOWS else 0)


def movers(axis, sign):
    return [q for q in range(POPS) if LATTICE[q][axis] == sign]


XP, XM = movers(0, 1), movers(0, -1)
YM = {1: movers(1, 1), -1: movers(1, -1)}
ZM = {1: movers(2, 1), -1: movers(2, -1)}
FACE = len(XP)
ORDER = XP + XM + [q for q in range(POPS) if LATTICE[q][0] == 0]
POS = {q: i for i, q in enumerate(ORDER)}
XY = [q for q in range(FLOWS) if LATTICE[q][0] != 0 and LATTICE[q][1] != 0]
XZ = [q for q in range(FLOWS) if LATTICE[q][0] != 0 and LATTICE[q][2] != 0]
LANE0 = 8


def messages():
    out = [("xz", q, LATTICE[q]) for q in XZ]
    out += [("xy", q, LATTICE[q]) for q in XY]
    out += [("x", 1, (1, 0, 0)), ("x", -1, (-1, 0, 0))]
    out += [("yz", (cz, cy), (0, cy, cz)) for cz in (1, -1) for cy in (1, -1)]
    out += [("z", cz, (0, 0, cz)) for cz in (1, -1)]
    out += [("y", 1, (0, 1, 0)), ("y", -1, (0, -1, 0))]
    return out


MESSAGES = messages()
EDGE = {m[:2]: i for i, m in enumerate(m for m in MESSAGES if m[0] in ("xy", "yz"))}
END_PLANES = ("x", "xy", "xz")
ALL_PLANES = ("y", "z", "yz")


def collide(f):
    s, d = {}, {}
    for q in range(1, FLOWS, 2):
        s[q] = f[q] + f[q + 1]
        d[q] = f[q] - f[q + 1]
    rho = (((s[1] + s[3]) + (s[5] + s[7])) + ((s[9] + s[11]) + (s[13] + s[15]))) + (s[17] + f[0])
    jx = (d[1] + d[7]) + (d[9] + d[11]) + d[13]
    jy = (d[3] + d[7]) + (d[15] + d[17]) - d[9]
    jz = (d[5] + d[11]) + (d[15] - d[13]) - d[17]
    g = [f[FLOWS + i] for i in range(7)]
    warmth = ((g[0] + g[1]) + (g[2] + g[3])) + ((g[4] + g[5]) + g[6])
    force = GRAVITY_LIFT * rho * warmth
    inv = 1.0 / rho
    ux = jx * inv
    uy = jy * inv
    uz = (jz + 0.5 * force) * inv

    w2 = 1.0 / 36.0
    keep = 1.0 - 1.0 / TAU_FLOW
    r = (w2 / TAU_FLOW) * rho
    sf = (w2 * (1.0 - 0.5 / TAU_FLOW)) * force
    r3 = 3.0 * r
    rx, ry, rz = r3 * ux, r3 * uy, r3 * uz
    sf3 = 3.0 * sf
    ax, ay, az = rx, ry, rz + sf3
    bx, by, bz = 1.5 * rx, 1.5 * ry, 1.5 * rz + 3.0 * sf3
    qx, qy, qz = ux * bx, uy * by, uz * bz
    usq = rx * ux + ry * uy + rz * uz
    base = r - 0.5 * usq - sf3 * uz
    cxy = ux * by + uy * bx
    cxz = ux * bz + uz * bx
    cyz = uy * bz + uz * by

    out = {0: keep * f[0] + 12.0 * base}

    def pair(q, even, odd):
        out[q] = keep * f[q] + (even + odd)
        out[q + 1] = keep * f[q + 1] + (even - odd)

    pair(1, 2.0 * (base + qx), 2.0 * ax)
    pair(3, 2.0 * (base + qy), 2.0 * ay)
    pair(5, 2.0 * (base + qz), 2.0 * az)
    exy = base + (qx + qy)
    exz = base + (qx + qz)
    eyz = base + (qy + qz)
    pair(7, exy + cxy, ax + ay)
    pair(9, exy - cxy, ax - ay)
    pair(11, exz + cxz, ax + az)
    pair(13, exz - cxz, ax - az)
    pair(15, eyz + cyz, ay + az)
    pair(17, eyz - cyz, ay - az)

    keep_heat = 1.0 - 1.0 / TAU_HEAT
    t8 = (0.125 / TAU_HEAT) * warmth
    t2 = 4.0 * t8
    out[FLOWS] = keep_heat * g[0] + 2.0 * t8
    for i, u in ((1, ux), (3, uy), (5, uz)):
        odd = t2 * u
        out[FLOWS + i] = keep_heat * g[i] + (t8 + odd)
        out[FLOWS + i + 1] = keep_heat * g[i + 1] + (t8 - odd)
    return out


def flux(f):
    total = lambda values: functools.reduce(lambda a, b: a + b, values)
    rho = total([f[q] for q in range(FLOWS)])
    jz = total([f[q] for q in range(FLOWS) if LATTICE[q][2] == 1]) - total(
        [f[q] for q in range(FLOWS) if LATTICE[q][2] == -1]
    )
    warmth = total([f[q] for q in range(FLOWS, POPS)])
    force = GRAVITY_LIFT * rho * warmth
    return (jz + 0.5 * force) / rho * warmth


def kernel(
    shape,
    sizes,
    flow_in,
    heat_in,
    flow_out,
    heat_out,
    total,
    held,
    post,
    ysend,
    yrecv,
    zsend,
    zrecv,
    zdiag,
    edge_send,
    edge_recv,
    part,
    parts,
    in_sem,
    send_sem,
    recv_sem,
    part_send,
    part_recv,
    total_send,
    total_recv,
):
    nx, ny, nz = shape
    planes, rows, lanes = sizes
    me = tuple(lax.axis_index(a) for a in AXES)
    count = nx * ny * nz
    group = ny * nz
    lines = nx - nx // 4
    my_index = me[0] * group + me[1] * nz + me[2]
    is_root = me[0] < lines

    def at(off):
        return tuple(m if d == 0 else lax.rem(m + (d % n), n) for m, d, n in zip(me, off, shape))

    offsets = [off for off in np.ndindex(3, 3, 3) if off != (1, 1, 1)]
    offsets = [tuple(d - 1 for d in off) for off in offsets if 1 in off]
    offsets.sort(key=lambda off: -2 * abs(off[0]) - abs(off[2]))
    barrier = pltpu.get_barrier_semaphore()
    for off in offsets:
        pl.semaphore_signal(barrier, inc=1, device_id=at(off), device_id_type=MESH)

    inner, ends = range(1, planes - 1), (0, planes - 1)
    blocks = [(0, 1), (planes - 1, 1), (1, planes - 2)]
    loads = []
    for i, (x, n) in enumerate(blocks):
        some = pl.ds(x * rows, n * rows)
        for j, (ref, low, n) in enumerate(((flow_in, 0, FLOWS), (heat_in, FLOWS, 7))):
            loads.append(
                pltpu.make_async_copy(ref.at[:, some], held.at[pl.ds(low, n), some], in_sem.at[2 * i + j])
            )
    for c in loads:
        c.start()

    far = range(STEPS + 2, nx - STEPS - 1)
    greeters = sum((lax.rem(me[0] + nx - d, nx) < lines).astype(jnp.int32) for d in far)

    @pl.when(is_root)
    def _():
        for d in far:
            pl.semaphore_signal(barrier, inc=1, device_id=at((d, 0, 0)), device_id_type=MESH)

    lane = lax.broadcasted_iota(jnp.int32, (rows, lanes), 1)
    row = lax.broadcasted_iota(jnp.int32, (rows, lanes), 0)
    is_bottom = me[2] == 0
    is_top = me[2] == nz - 1
    end_lane = {1: lane == 0, -1: lane == lanes - 1}
    wall = {1: jnp.logical_and(end_lane[1], is_bottom), -1: jnp.logical_and(end_lane[-1], is_top)}
    end_row = {1: row == 0, -1: row == rows - 1}
    far_row = {1: rows - 1, -1: 0}
    side = {1: 0, -1: 1}

    def turn(v, c, axis):
        n = rows if axis == 0 else lanes
        return pltpu.roll(v, 1 if c == 1 else n - 1, axis)

    def plane(x):
        return pl.ds((x + 1) * rows, rows)

    def keep(s, x, out, packed):
        if x in ends:
            cx = 1 if x else -1
            for q in XY:
                if LATTICE[q][0] == cx:
                    far = far_row[LATTICE[q][1]]
                    edge_send[s, EDGE["xy", q]] = out[q][far : far + 1, :]
        for q in range(POPS):
            post[s, POS[q], plane(x), :] = out[q]
        for cz in (1, -1):
            for j, q in enumerate(ZM[cz]):
                k = LANE0 + j * planes + x
                packed[cz] = jnp.where(lane == k, pltpu.roll(out[q], k + (1 if cz == 1 else 0), 1), packed[cz])

    def crew(end, dz):
        return (0 if end else 3) + dz + 1

    def copy(s, m):
        kind, slot, off = MESSAGES[m]
        if kind == "x":
            some = pl.ds(0 if slot == 1 else FACE, FACE)
            src, dst = (planes - 1, -1) if slot == 1 else (0, planes)
            src, dst = post.at[s, some, plane(src)], post.at[s, some, plane(dst)]
        elif kind == "y":
            src, dst = ysend.at[s, side[slot]], yrecv.at[s, side[slot]]
        elif kind == "z":
            src, dst = zsend.at[s, side[slot]], zrecv.at[s, side[slot]]
        elif kind == "xz":
            src = post.at[s, POS[slot], plane(planes - 1 if off[0] == 1 else 0)]
            dst = zdiag.at[s, XZ.index(slot)]
        else:
            src, dst = edge_send.at[s, EDGE[kind, slot]], edge_recv.at[s, EDGE[kind, slot]]
        return pltpu.make_async_remote_copy(
            src_ref=src,
            dst_ref=dst,
            send_sem=send_sem.at[s, crew(kind in END_PLANES, off[2])],
            recv_sem=recv_sem.at[s, crew(kind in END_PLANES, off[2])],
            device_id=at(off),
            device_id_type=MESH,
        )

    def of_kind(kinds, dz):
        return [m for m, (kind, _, off) in enumerate(MESSAGES) if kind in kinds and off[2] == dz]

    def each(act, up, down):
        for dz, when in ((1, up), (-1, down)):

            @pl.when(when)
            def _():
                act(dz)

        act(0)

    def start(s, kinds):
        def act(dz):
            for m in of_kind(kinds, dz):
                copy(s, m).start()

        each(act, jnp.logical_not(is_top), jnp.logical_not(is_bottom))

    def bytes_of(s, kinds, dz):
        size = {"x": FACE * rows, "y": FACE * planes, "z": rows, "xz": rows, "xy": 1, "yz": 1}
        some = parts.at[pl.ds(0, sum(size[MESSAGES[m][0]] for m in of_kind(kinds, dz)))]
        return pltpu.make_async_remote_copy(
            src_ref=some,
            dst_ref=some,
            send_sem=send_sem.at[s, crew(kinds == END_PLANES, dz)],
            recv_sem=recv_sem.at[s, crew(kinds == END_PLANES, dz)],
            device_id=at((1, 0, 0)),
            device_id_type=MESH,
        )

    def receive(s, kinds):
        each(lambda dz: bytes_of(s, kinds, dz).wait_recv(), jnp.logical_not(is_bottom), jnp.logical_not(is_top))

    def drain(s, kinds):
        each(lambda dz: bytes_of(s, kinds, dz).wait_send(), jnp.logical_not(is_top), jnp.logical_not(is_bottom))

    def pack(s, packed):
        for cy in (1, -1):
            first = rows + far_row[cy]
            for j, q in enumerate(YM[cy]):
                ysend[s, side[cy], j] = post[s, POS[q], pl.ds(first, planes, stride=rows), :]
        for cz in (1, -1):
            zsend[s, side[cz]] = packed[cz]
            for cy in (1, -1):
                far = far_row[cy]
                edge_send[s, EDGE["yz", (cz, cy)]] = packed[cz][far : far + 1, :]

    def z_faces(s):
        tiles = {}
        for cz in (1, -1):
            own = zrecv[s, side[cz]]
            tiles[cz, 0] = own
            for cy in (1, -1):
                other = jnp.broadcast_to(edge_recv[s, EDGE["yz", (cz, cy)]], (rows, lanes))
                tiles[cz, cy] = jnp.where(end_row[cy], other, turn(own, cy, 0))
        return tiles

    def stream(s, x, tiles):
        f = {}
        for q in range(POPS):
            cx, cy, cz = LATTICE[q]
            v = post[s, POS[q], plane(x - cx), :]
            inside = 0 <= x - cx < planes
            if cy:
                if inside:
                    edge = yrecv[s, side[cy], YM[cy].index(q), pl.ds(x - cx, 1), :]
                else:
                    edge = edge_recv[s, EDGE["xy", q]]
                v = jnp.where(end_row[cy], jnp.broadcast_to(edge, (rows, lanes)), turn(v, cy, 0))
            if cz:
                if inside:
                    k = LANE0 + ZM[cz].index(q) * planes + x - cx
                    edge = pltpu.roll(tiles[cz, cy], (lanes if cz == 1 else lanes - 1) - k, 1)
                else:
                    edge = turn(zdiag[s, XZ.index(q)], cz, 1)
                back = post[s, POS[opposite(q)], plane(x), :]
                if q >= FLOWS:
                    back = 0.25 * (HOT_WALL if cz == 1 else COLD_WALL) - back
                v = jnp.where(wall[cz], back, jnp.where(end_lane[cz], edge, turn(v, cz, 1)))
            f[q] = v
        return f

    blank = jnp.zeros((rows, lanes), jnp.float32)

    def first(x, packed):
        keep(0, x, collide({q: held[q, pl.ds(x * rows, rows), :] for q in range(POPS)}), packed)

    packed = {1: blank, -1: blank}
    for c in loads[:4]:
        c.wait()
    for x in ends:
        first(x, packed)
    pl.semaphore_wait(barrier, len(offsets) + greeters)
    start(0, END_PLANES)
    for c in loads[4:]:
        c.wait()
    for x in inner:
        first(x, packed)
    pack(0, packed)
    start(0, ALL_PLANES)

    for s in range(1, STEPS):
        packed = {1: blank, -1: blank}
        receive(s - 1, ALL_PLANES)
        tiles = z_faces(s - 1)
        for x in inner:
            keep(s, x, collide(stream(s - 1, x, tiles)), packed)
        receive(s - 1, END_PLANES)
        for x in ends:
            keep(s, x, collide(stream(s - 1, x, tiles)), packed)
        start(s, END_PLANES)
        pack(s, packed)
        start(s, ALL_PLANES)

    def last(x, tiles):
        f = stream(STEPS - 1, x, tiles)
        for q in range(FLOWS):
            flow_out[q, pl.ds(x * rows, rows), :] = f[q]
        for q in range(FLOWS, POPS):
            heat_out[q - FLOWS, pl.ds(x * rows, rows), :] = f[q]
        return flux(f)

    receive(STEPS - 1, ALL_PLANES)
    tiles = z_faces(STEPS - 1)
    acc = blank
    for x in inner:
        acc = acc + last(x, tiles)
    receive(STEPS - 1, END_PLANES)
    for x in ends:
        acc = acc + last(x, tiles)

    mine = jnp.sum(acc, axis=0, keepdims=True)
    part[0] = mine
    parts[my_index] = mine
    seat = lax.rem(my_index, group)

    def to_root(x, d):
        return pltpu.make_async_remote_copy(
            src_ref=part.at[0],
            dst_ref=parts.at[my_index],
            send_sem=part_send.at[0],
            recv_sem=part_recv.at[0],
            device_id=x * group + lax.rem(seat + d, group),
            device_id_type=pl.DeviceIdType.LOGICAL,
        )

    for x in range(lines):

        @pl.when(me[0] != x)
        def _():
            to_root(x, 0).start()

        for d in range(1, group):
            to_root(x, d).start()

    serves = jnp.logical_and(me[0] >= nx // 2, is_root)
    served = [nx + nx // 2 - 1 - me[0]]

    def to_served(i):
        return pltpu.make_async_remote_copy(
            src_ref=total.at[0],
            dst_ref=total.at[0],
            send_sem=total_send.at[i],
            recv_sem=total_recv.at[0],
            device_id=(served[i], me[1], me[2]),
            device_id_type=MESH,
        )

    def whole(n, k):
        some = parts.at[pl.ds(0, n)]
        return pltpu.make_async_remote_copy(
            src_ref=some,
            dst_ref=some,
            send_sem=part_send.at[k],
            recv_sem=part_recv.at[0],
            device_id=0,
            device_id_type=pl.DeviceIdType.LOGICAL,
        )

    for s in range(STEPS):
        drain(s, END_PLANES)
        drain(s, ALL_PLANES)

    @pl.when(is_root)
    def _():
        whole(lines * group - 1, 0).wait_send()

    @pl.when(jnp.logical_not(is_root))
    def _():
        whole(lines * group, 0).wait_send()

    @pl.when(is_root)
    def _():
        whole(count - 1, 0).wait_recv()
        sums = [parts[i] for i in range(8)]
        for i in range(8, count):
            sums[i % 8] = sums[i % 8] + parts[i]
        total[0] = ((sums[0] + sums[1]) + (sums[2] + sums[3])) + ((sums[4] + sums[5]) + (sums[6] + sums[7]))

        @pl.when(serves)
        def _():
            to_served(0).start()

    @pl.when(jnp.logical_not(is_root))
    def _():
        to_served(0).wait_recv()

    @pl.when(serves)
    def _():
        to_served(0).wait_send()


def write_out(scale, flow, heat, total, flow_out, heat_out, nusselt, value, sem):
    copies = [
        pltpu.make_async_copy(flow, flow_out, sem.at[0]),
        pltpu.make_async_copy(heat, heat_out, sem.at[1]),
    ]
    for c in copies:
        c.start()
    value[...] = 1.0 + scale * jnp.sum(total[0], axis=1, keepdims=True)
    copies.append(pltpu.make_async_copy(value, nusselt, sem.at[2]))
    copies[2].start()
    for c in copies:
        c.wait()


def per_device(shape, flow_pops, heat_pops):
    nx, ny, nz = shape
    _, planes, rows, lanes = flow_pops.shape
    flat = (planes * rows, lanes)
    dma = pltpu.SemaphoreType.DMA
    tile = (rows, lanes)
    vmem = lambda *dims: pltpu.VMEM(dims, jnp.float32)
    anywhere = pl.BlockSpec(memory_space=pl.ANY)
    in_vmem = pl.BlockSpec(memory_space=pltpu.VMEM)
    state = pl.pallas_call(
        functools.partial(kernel, shape, (planes, rows, lanes)),
        out_shape=(
            vmem(FLOWS, *flat),
            vmem(7, *flat),
            vmem(1, 1, lanes),
        ),
        in_specs=[anywhere] * 2,
        out_specs=(in_vmem,) * 3,
        scratch_shapes=[
            vmem(POPS, *flat),
            vmem(STEPS, POPS, (planes + 2) * rows, lanes),
            vmem(STEPS, 2, FACE, *tile),
            vmem(STEPS, 2, FACE, *tile),
            vmem(STEPS, 2, *tile),
            vmem(STEPS, 2, *tile),
            vmem(STEPS, len(XZ), *tile),
            vmem(STEPS, len(EDGE), 1, lanes),
            vmem(STEPS, len(EDGE), 1, lanes),
            vmem(1, 1, lanes),
            vmem(max(nx * ny * nz, 128), 1, lanes),
            dma((6,)),
            dma((STEPS, 6)),
            dma((STEPS, 6)),
            dma((1,)),
            dma((1,)),
            dma((1,)),
            dma((1,)),
        ],
        compiler_params=pltpu.CompilerParams(collective_id=0, has_side_effects=True),
        name="lattice_steps",
    )(flow_pops.reshape((FLOWS,) + flat), heat_pops.reshape((7,) + flat))
    cells = nx * ny * nz * planes * rows * lanes
    scale = nz * lanes / (DIFFUSIVITY * (HOT_WALL - COLD_WALL)) / cells
    flow, heat, nusselt = pl.pallas_call(
        functools.partial(write_out, scale),
        out_shape=(
            jax.ShapeDtypeStruct((FLOWS,) + flat, jnp.float32),
            jax.ShapeDtypeStruct((7,) + flat, jnp.float32),
            jax.ShapeDtypeStruct((1, 1), jnp.float32),
        ),
        in_specs=[in_vmem] * 3,
        out_specs=(anywhere,) * 3,
        scratch_shapes=[vmem(1, 1), dma((3,))],
        name="write_out",
    )(*(pltpu.with_memory_space_constraint(a, pltpu.VMEM) for a in state))
    return flow.reshape(flow_pops.shape), heat.reshape(heat_pops.shape), nusselt.reshape(())


def solution(mesh):
    shape = tuple(mesh.shape[a] for a in AXES)
    spec = P(None, *AXES)
    return jax.shard_map(
        functools.partial(per_device, shape),
        mesh=mesh,
        in_specs=(spec, spec),
        out_specs=(spec, spec, P()),
        check_vma=False,
    )
```
